256 devices in a mesh: area: 32 (over y, x, core), rank: 8 (over z).
Axes of the slice: x: 4, y: 4, z: 8, core: 2. Of those that a mesh axis runs over, the one named last changes fastest.
Arguments:
- initial_bits: int32 [2, 48, 1024], P(None, None, ('area', 'rank')), may hold values from -2147483648 to 2147483646
- membrane: float32 [48, 32768], P(None, ('area', 'rank')), may hold values from -100 to 200
- drive: int32 [32768], P(('area', 'rank')), may hold values from 0 to 47
- leak_shift: int32 [32768], P(('area', 'rank')), may hold values from 2 to 5
- weights: bfloat16 [256, 128, 128, 128], P(('area', 'rank')), may hold values from -3 to 3, as said below
- pre_block: int32 [256, 128], P(('area', 'rank')), may hold values from 0 to 255
- block_mask: int32 [256, 128], P(('area', 'rank')), may hold values 0 or 1
- delay: int32 [256, 128], P(('area', 'rank')), may hold values from 2 to 5
- area_of_block: int32 [256, 1], replicated, may hold values from 0 to 31
Outputs:
- final_membrane: float32 [48, 32768], P(None, ('area', 'rank'))
- area_rates: float32 [10, 32], replicated
The draws below stay inside these ranges and needn't reach their ends.
Inputs may be any that keep to these rules, and one draw needn't show every extreme that they name: weights hold whole numbers. `area_of_block`: every area holds at least one block.
All inputs are finite; a program needn't handle non-finite values. No bound on the sum of `block_mask` on one device may be relied on, other than what follows from the above.
Results may differ from the reference program's by a relative error of at most 0.0003.
Values sent between devices are 32-bit elements; how exact they have to be, the bound alone decides.
No kernel may reach another device: no remote copies, remote signals or barrier semaphores. Data moves between devices by JAX's collectives and lax.ppermute only.
A program may use at most 128 MiB of HBM per device.

```python
import jax
import jax.numpy as jnp
from jax import lax

BLOCK = 128
AREAS = 32
K = 128
TRIALS = 48
DMIN = 2
NDELAY = 4
STEPS = 10
BLOCKS = 256
NEURONS = 32768


def draw_weights(key, part):
    values = jax.random.randint(key, (BLOCKS, K, BLOCK, BLOCK), -3, 4)
    return values.astype(jnp.float32).astype(jnp.bfloat16)


def with_ends(result, stream_key, smallest, top_value):
    extent = result.shape
    index_at = [jax.random.randint(jax.random.fold_in(stream_key, axis), (), 0, extent[axis]) for axis in range(len(extent))]
    result = result.at[tuple(index_at)].set(smallest)
    longest = extent.index(max(extent))
    index_at[longest] = (index_at[longest] + 1) % extent[longest]
    return result.at[tuple(index_at)].set(top_value)


def block_levels(stream_key, shape, shards, smallest, largest):
    def one(position, shards_of):
        draws = jax.random.uniform(jax.random.fold_in(jax.random.fold_in(stream_key, 6), position), (shards_of,), jnp.float32, smallest / len(shards), largest / len(shards))
        return jnp.repeat(jnp.exp(draws), shape[position] // shards_of).reshape((-1,) + (1,) * (len(shape) - position - 1))

    gain = one(*shards[0])
    for cut in shards[1:]:
        gain = gain * one(*cut)
    return gain


def different_ones(own_key, rows, amount, top, lift):
    ranking = jax.random.permutation(jax.random.fold_in(own_key, 1), amount)
    favour = ranking
    for power in range(3):
        favour = favour * favour // amount
    favour = favour * lift // amount
    tickets = jax.random.randint(jax.random.fold_in(own_key, 2), (rows, amount), 0, 4096) + favour
    sure = jax.random.permutation(jax.random.fold_in(own_key, 3), rows)[jnp.arange(amount) % rows]
    tickets = jnp.where(jnp.arange(rows)[:, None] == sure[None, :], 1 << 14, tickets)
    merit = tickets * amount + jnp.arange(amount)
    return lax.top_k(merit.astype(jnp.int32), top)[1].astype(jnp.int32)


def setup_inputs(seed: int = 0) -> dict:
    arg_keys = jax.random.split(jax.random.key(seed), 10)
    initial_bits = with_ends(jax.random.randint(arg_keys[0], (DMIN, TRIALS, NEURONS // 32), -2147483648, 2147483647), jax.random.fold_in(arg_keys[0], 1), -2147483648, 2147483646).astype(jnp.int32)
    membrane = jnp.clip(-100.0 + 300.0 * jax.random.uniform(arg_keys[1], (TRIALS, NEURONS), jnp.float32) ** block_levels(arg_keys[1], (TRIALS, NEURONS), ((1, 256),), -0.2, 0.2), -100.0, 200.0)
    drive = with_ends(jax.random.randint(arg_keys[2], (NEURONS,), 0, 48), jax.random.fold_in(arg_keys[2], 1), 0, 47).astype(jnp.int32)
    leak_shift = with_ends(jax.random.randint(arg_keys[3], (NEURONS,), 2, 6), jax.random.fold_in(arg_keys[3], 1), 2, 5).astype(jnp.int32)
    weights = draw_weights(jax.random.fold_in(arg_keys[9], 71), 0)
    pre_block = with_ends(jax.random.randint(arg_keys[5], (BLOCKS, K), 0, BLOCKS), jax.random.fold_in(arg_keys[5], 1), 0, BLOCKS - 1).astype(jnp.int32)
    block_mask = with_ends((jax.random.randint(arg_keys[6], (BLOCKS, K), 0, 4) < 3).astype(jnp.int32), jax.random.fold_in(arg_keys[6], 1), 0, 1)
    delay = with_ends(jax.random.randint(arg_keys[7], (BLOCKS, K), DMIN, DMIN + NDELAY), jax.random.fold_in(arg_keys[7], 1), DMIN, (DMIN + NDELAY) - 1).astype(jnp.int32)
    area_of_block = different_ones(arg_keys[8], BLOCKS, AREAS, 1, 512)
    return dict(initial_bits=initial_bits, membrane=membrane, drive=drive, leak_shift=leak_shift, weights=weights, pre_block=pre_block, block_mask=block_mask, delay=delay, area_of_block=area_of_block)


threshold_level = 200.0


def unpack(packed):
    shifts = jnp.arange(32, dtype=jnp.int32)
    bit_values = jnp.bitwise_and(jnp.right_shift(packed[..., None], shifts), 1)
    return bit_values.reshape(packed.shape[:-1] + (packed.shape[-1] * 32,))


def reference(initial_bits, membrane, drive, leak_shift, weights, pre_block, block_mask, delay, area_of_block):
    neurons = BLOCKS * BLOCK
    intervals = STEPS // DMIN
    lag_table = (delay[:, :, None] - DMIN == jnp.arange(NDELAY, dtype=jnp.int32)[None, None, :]).astype(jnp.float32)
    input_weighting = block_mask.astype(jnp.float32)[:, :, None] * lag_table
    buffer = jnp.zeros((STEPS + NDELAY, TRIALS, neurons), jnp.float32)
    history = unpack(initial_bits).astype(jnp.float32)
    membrane_voltage = jnp.floor(membrane)
    leak_scale = 1.0 / jnp.left_shift(jnp.ones_like(leak_shift), leak_shift).astype(jnp.float32)
    drive_float = drive.astype(jnp.float32)
    area_table = (area_of_block[:, 0:1] == jnp.arange(AREAS, dtype=jnp.int32)[None, :]).astype(jnp.float32)
    block_counts = []
    for interval in range(intervals):
        source_rows = history.reshape(DMIN * TRIALS, BLOCKS, BLOCK)

        def one_block(operands):
            synapses, source, delay_weight_table = operands
            selected = jnp.take(source_rows, source, axis=1).astype(jnp.float32)
            product = jnp.einsum("rkm,kmn->krn", selected, synapses.astype(jnp.float32), precision=lax.Precision.HIGHEST)
            return jnp.einsum("kd,krn->drn", delay_weight_table, product, precision=lax.Precision.HIGHEST)

        arrived = lax.map(one_block, (weights, pre_block, input_weighting))
        arrived = arrived.reshape(BLOCKS, NDELAY, DMIN, TRIALS, BLOCK)
        arrived = jnp.transpose(arrived, (1, 2, 3, 0, 4)).reshape(NDELAY, DMIN, TRIALS, neurons)
        first_step = (interval - 1) * DMIN
        for lag_index in range(NDELAY):
            for offset in range(DMIN):
                landing = first_step + offset + DMIN + lag_index
                buffer = buffer.at[landing].add(arrived[lag_index, offset])
        fired_list = []
        for offset in range(DMIN):
            current = buffer[interval * DMIN + offset]
            membrane_voltage = membrane_voltage - jnp.floor(membrane_voltage * leak_scale) + current + drive_float
            current_spike_flags = membrane_voltage >= threshold_level
            membrane_voltage = jnp.where(current_spike_flags, jnp.zeros_like(membrane_voltage), jnp.maximum(membrane_voltage, -threshold_level))
            spikes = current_spike_flags.astype(jnp.float32)
            fired_list.append(spikes)
            block_counts.append(jnp.sum(spikes.reshape(TRIALS, BLOCKS, BLOCK), axis=(0, 2)))
        history = jnp.stack(fired_list)
    counts = jnp.dot(jnp.stack(block_counts), area_table, precision=lax.Precision.HIGHEST)
    sizes_per_area = jnp.sum(area_table, axis=0) * (TRIALS * BLOCK)
    return membrane_voltage, counts / sizes_per_area
```

```python
import jax
import jax.numpy as jnp
from jax import lax
from jax.experimental import pallas as pl
from jax.experimental.pallas import tpu as pltpu
from jax.sharding import Mesh
from jax.sharding import PartitionSpec as P

AREAS = 32
DMIN = 2
NDELAY = 4
STEPS = 10
BLOCK = 128
TRIALS = 48
SLOTS = 128
THRESHOLD = 200.0
GROUP = 16
WORDS = 3
HALF = 128 * WORDS
TABLE = 2 * HALF
AREA_RANK = ("area_0", "area_1", "area_2", "rank")
PLANE = ("area_0", "area_1", "rank")

VMEM = pl.BlockSpec(memory_space=pltpu.VMEM)
SMEM = pl.BlockSpec(memory_space=pltpu.SMEM)


def kernel_call(body, outs, ins, scratch, name, limit):
    return pl.pallas_call(
        body,
        out_shape=outs,
        in_specs=ins,
        out_specs=jax.tree.map(lambda _: VMEM, outs),
        scratch_shapes=scratch,
        name=name,
        compiler_params=pltpu.CompilerParams(vmem_limit_bytes=limit << 20),
    )


def row_ids(rows, lanes=BLOCK):
    return lax.broadcasted_iota(jnp.int32, (rows, lanes), 0)


def lane_ids(rows, lanes=BLOCK):
    return lax.broadcasted_iota(jnp.int32, (rows, lanes), 1)


def words_of(spikes):
    words = []
    for j in range(WORDS):
        bits = jnp.zeros((8, BLOCK), jnp.int32)
        for step in range(DMIN):
            for part in range(2):
                shift = row_ids(8) + (8 * part + 16 * step)
                flags = spikes[step][16 * j + 8 * part : 16 * j + 8 * part + 8]
                bits = bits | jnp.where(flags, jnp.left_shift(1, shift), 0)
        words.append(jnp.sum(bits, axis=0, keepdims=True, dtype=jnp.int32))
    return words


def store_copies(out_ref, words):
    which = row_ids(24) % WORDS
    rows = jnp.where(which == 0, words[0], jnp.where(which == 1, words[1], words[2]))
    for copy in range(HALF // 24):
        out_ref[pl.ds(24 * copy, 24), :] = rows


def first_body(bits_ref, out_ref):
    spikes = []
    lane = lane_ids(TRIALS)
    for step in range(DMIN):
        packed = bits_ref[step]
        word = jnp.zeros((TRIALS, BLOCK), jnp.int32)
        for w in range(BLOCK // 32):
            word = jnp.where(lane // 32 == w, packed[:, w : w + 1], word)
        spikes.append(jnp.bitwise_and(jnp.right_shift(word, lane % 32), 1) == 1)
    store_copies(out_ref, words_of(spikes))


def shifted(older, newer):
    return lax.shift_right_logical(older, 16) | jnp.left_shift(newer, 16)


def interval_body(number, n_hist):
    last = number == STEPS // DMIN - 1

    def body(index_ref, *refs):
        hist = refs[: 2 * n_hist]
        w_ref, v_ref, drive_ref, leak_ref, count_ref = refs[2 * n_hist : 2 * n_hist + 5]
        v_out, pk_out, count_out, table, lhs = refs[2 * n_hist + 5 :]

        for half in range(2):
            at = [hist[2 * a + half][...] if a < n_hist else None for a in range(3)]
            for lag in range(NDELAY):
                newer = at[lag // 2]
                if lag % 2:
                    older = at[lag // 2 + 1]
                    if newer is None:
                        rows = None
                    elif older is None:
                        rows = jnp.left_shift(newer, 16)
                    else:
                        rows = shifted(older, newer)
                else:
                    rows = newer
                if rows is None:
                    rows = jnp.zeros((HALF, BLOCK), jnp.int32)
                table[pl.ds(lag * TABLE + half * HALF, HALF), :] = rows
        table[pl.ds(NDELAY * TABLE, 8), :] = jnp.zeros((8, BLOCK), jnp.int32)

        shift = row_ids(32)

        def group(i, acc):
            for k in range(GROUP):
                base = index_ref[0, i * GROUP + k]
                for j in range(WORDS):
                    word = table[pl.ds(base + j, 1), :]
                    bit = jnp.bitwise_and(jnp.right_shift(word, shift), 1)
                    lhs[pl.ds(32 * j, 32), pl.ds(k * BLOCK, BLOCK)] = bit.astype(
                        jnp.float32
                    ).astype(jnp.bfloat16)
            part = w_ref[pl.ds(i * (GROUP * BLOCK), GROUP * BLOCK), :]
            return acc + jnp.dot(lhs[...], part, preferred_element_type=jnp.float32)

        zero = jnp.zeros((DMIN * TRIALS, BLOCK), jnp.float32)
        current = lax.fori_loop(0, SLOTS // GROUP, group, zero)

        v = v_ref[...]
        if number == 0:
            v = jnp.floor(v)
        drive = drive_ref[...].astype(jnp.float32)
        leak = 1.0 / jnp.left_shift(jnp.ones((1, BLOCK), jnp.int32), leak_ref[...]).astype(jnp.float32)
        spikes = []
        for step in range(DMIN):
            arrived = jnp.concatenate(
                [current[32 * j + 16 * step : 32 * j + 16 * step + 16] for j in range(WORDS)], axis=0
            )
            v = v - jnp.floor(v * leak) + arrived + drive
            fired = v >= THRESHOLD
            v = jnp.where(fired, 0.0, jnp.maximum(v, -THRESHOLD))
            spikes.append(fired)
        v_out[...] = v
        if not last:
            store_copies(pk_out, words_of(spikes))
        lane = lane_ids(8)
        counts = count_ref[...] if number else jnp.zeros((8, BLOCK), jnp.float32)
        for step in range(DMIN):
            total = jnp.sum(spikes[step].astype(jnp.float32), axis=0, keepdims=True)
            total = jnp.sum(total, axis=1, keepdims=True)
            counts = counts + jnp.where(lane == number * DMIN + step, total, 0.0)
        count_out[...] = counts
        if last:
            for copy in range(pk_out.shape[0] // 8):
                pk_out[pl.ds(8 * copy, 8), :] = counts

    return body


def rates_body(counts_ref, area_ref, out_ref):
    counts = counts_ref[...]
    table = (area_ref[...] == lane_ids(counts.shape[0])).astype(jnp.float32)
    sizes = jnp.sum(table, axis=0, keepdims=True) * float(TRIALS * BLOCK)
    sums = lax.dot_general(
        counts, table, (((0,), (0,)), ((), ())), precision=lax.Precision.HIGHEST,
        preferred_element_type=jnp.float32,
    )
    out_ref[...] = sums[:STEPS, :AREAS] / sizes[:, :AREAS]


def exchanged(copies, axes):
    rows = copies.shape[0]
    peers = lax.axis_size(axes)
    pieces = copies.reshape(peers, 1, rows // peers * BLOCK)
    return lax.all_to_all(pieces, axes, split_axis=0, concat_axis=0).reshape(rows, BLOCK)


def on_device(
    initial_bits, membrane, drive, leak_shift, weights, pre_block, block_mask, delay, area_of_block
):
    words = jax.ShapeDtypeStruct((HALF, BLOCK), jnp.int32)
    volts = jax.ShapeDtypeStruct((TRIALS, BLOCK), jnp.float32)
    totals = jax.ShapeDtypeStruct((8, BLOCK), jnp.float32)
    blocks = area_of_block.shape[0]

    core = lax.axis_index("area_2")
    ranks = lax.axis_size("rank")
    other = jnp.bitwise_xor(pre_block // ranks % 2, core)
    place = pre_block // (2 * ranks) * ranks + pre_block % ranks
    index = (delay - DMIN) * TABLE + other * HALF + place * WORDS
    index = jnp.where(block_mask == 1, index, NDELAY * TABLE)

    flat = weights.reshape(SLOTS * BLOCK, BLOCK)
    drive = drive.reshape(1, BLOCK)
    leak_shift = leak_shift.reshape(1, BLOCK)
    v = membrane
    counts = jnp.zeros((8, BLOCK), jnp.float32)
    copies = kernel_call(first_body, words, [VMEM], [], "first", 8)(initial_bits)
    hist = []
    for number in range(STEPS // DMIN):
        own = exchanged(copies, PLANE)
        partner = lax.ppermute(own, "area_2", [(0, 1), (1, 0)])
        hist = [(own, partner)] + hist[:2]
        last = number == STEPS // DMIN - 1
        out = jax.ShapeDtypeStruct((blocks, BLOCK), jnp.float32) if last else words
        v, copies, counts = kernel_call(
            interval_body(number, len(hist)),
            (volts, out, totals),
            [SMEM] + [VMEM] * (2 * len(hist) + 5),
            [
                pltpu.VMEM((NDELAY * TABLE + 8, BLOCK), jnp.int32),
                pltpu.VMEM((DMIN * TRIALS, GROUP * BLOCK), jnp.bfloat16),
            ],
            "interval",
            24,
        )(index, *[x for pair in hist for x in pair], flat, v, drive, leak_shift, counts)
    everyone = exchanged(copies, AREA_RANK)
    rates = jax.ShapeDtypeStruct((STEPS, AREAS), jnp.float32)
    rates = kernel_call(rates_body, rates, [VMEM, VMEM], [], "rates", 8)(everyone, area_of_block)
    return v, rates


def solution(mesh):
    split = Mesh(
        mesh.devices.reshape(4, 4, 2, mesh.shape["rank"]), ("area_0", "area_1", "area_2", "rank")
    )
    return jax.shard_map(
        on_device,
        mesh=split,
        in_specs=(
            P(None, None, AREA_RANK),
            P(None, AREA_RANK),
            P(AREA_RANK),
            P(AREA_RANK),
            P(AREA_RANK, None, None, None),
            P(AREA_RANK, None),
            P(AREA_RANK, None),
            P(AREA_RANK, None),
            P(),
        ),
        out_specs=(P(None, AREA_RANK), P()),
        check_vma=False,
    )
```

```python
import jax
import jax.numpy as jnp
from jax import lax
from jax.experimental import pallas as pl
from jax.experimental.pallas import tpu as pltpu
from jax.sharding import Mesh
from jax.sharding import PartitionSpec as P

AREAS = 32
DMIN = 2
NDELAY = 4
STEPS = 10
BLOCK = 128
TRIALS = 48
SLOTS = 128
THRESHOLD = 200.0
GROUP = 16
WORDS = 3
HALF = 128 * WORDS
TABLE = 2 * HALF
AREA_RANK = ("area_0", "area_1", "area_2", "rank")
PLANE = ("area_0", "area_1", "rank")

VMEM = pl.BlockSpec(memory_space=pltpu.VMEM)
SMEM = pl.BlockSpec(memory_space=pltpu.SMEM)
ANY = pl.BlockSpec(memory_space=pl.ANY)


def kernel_call(body, outs, ins, scratch, name, limit):
    return pl.pallas_call(
        body,
        out_shape=outs,
        in_specs=ins,
        out_specs=jax.tree.map(lambda _: VMEM, outs),
        scratch_shapes=scratch,
        name=name,
        compiler_params=pltpu.CompilerParams(vmem_limit_bytes=limit << 20),
    )


def row_ids(rows, lanes=BLOCK):
    return lax.broadcasted_iota(jnp.int32, (rows, lanes), 0)


def lane_ids(rows, lanes=BLOCK):
    return lax.broadcasted_iota(jnp.int32, (rows, lanes), 1)


def words_of(spikes):
    words = []
    for j in range(WORDS):
        bits = jnp.zeros((8, BLOCK), jnp.int32)
        for step in range(DMIN):
            for part in range(2):
                shift = row_ids(8) + (8 * part + 16 * step)
                flags = spikes[step][16 * j + 8 * part : 16 * j + 8 * part + 8]
                bits = bits | jnp.where(flags, jnp.left_shift(1, shift), 0)
        words.append(jnp.sum(bits, axis=0, keepdims=True, dtype=jnp.int32))
    return words


def store_copies(out_ref, words):
    which = row_ids(24) % WORDS
    rows = jnp.where(which == 0, words[0], jnp.where(which == 1, words[1], words[2]))
    for copy in range(HALF // 24):
        out_ref[pl.ds(24 * copy, 24), :] = rows


def first_body(bits_ref, out_ref):
    trial = lane_ids(8, TRIALS)
    which = row_ids(8, TRIALS)
    place = jnp.left_shift(1, trial % 16).astype(jnp.float32)
    places = jnp.where(trial // 16 == which, place, 0.0).astype(jnp.bfloat16)
    packed = jnp.zeros((8, BLOCK), jnp.int32)
    shift = row_ids(32, TRIALS)
    for step in range(DMIN):
        bits = [
            jnp.bitwise_and(jnp.right_shift(bits_ref[step, w : w + 1, :], shift), 1)
            for w in range(BLOCK // 32)
        ]
        bits = jnp.concatenate(bits, axis=0).astype(jnp.float32).astype(jnp.bfloat16)
        half = lax.dot_general(
            places, bits, (((1,), (1,)), ((), ())), preferred_element_type=jnp.float32
        )
        packed = packed | jnp.left_shift(half.astype(jnp.int32), 16 * step)
    store_copies(out_ref, [packed[j : j + 1] for j in range(WORDS)])


def plan_body(ranks, core_ref, pre_ref, mask_ref, delay_ref, after_ref, out_ref):
    pre = pre_ref[...]
    lag = delay_ref[...] - DMIN
    other = jnp.bitwise_xor(pre // ranks % 2, core_ref[0, 0])
    place = pre // (2 * ranks) * ranks + pre % ranks
    base = lag * TABLE + other * HALF + place * WORDS
    code = base * SLOTS + lane_ids(1)
    late = jnp.where((other == 1) & (lag < 2), 1, 0)
    kind = jnp.where(mask_ref[...] == 1, late, 2)

    def column(row):
        return jnp.transpose(jnp.broadcast_to(row, (SLOTS, SLOTS)))

    sub, lane = row_ids(SLOTS), lane_ids(SLOTS)
    kind_col, code_col = column(kind), column(code)
    kind_row = jnp.broadcast_to(kind, (SLOTS, SLOTS))
    before = jnp.where((kind_row == kind_col) & (lane < sub), 1, 0)
    rank_col = jnp.sum(before, axis=1, keepdims=True, dtype=jnp.int32)
    nothing = NDELAY * TABLE * SLOTS
    lane8 = lane_ids(8)
    row8 = row_ids(8)
    out = jnp.zeros((8, SLOTS), jnp.int32)
    for k in range(2):
        hit = (kind_col == k) & (rank_col == lane)
        codes = jnp.sum(jnp.where(hit, code_col - nothing, 0), axis=0, keepdims=True, dtype=jnp.int32)
        count = jnp.sum(jnp.where(kind == k, 1, 0), axis=1, keepdims=True, dtype=jnp.int32)
        out = jnp.where(row8 == k, codes + nothing, out)
        out = jnp.where((row8 == 2) & (lane8 == k), count, out)
    out_ref[...] = out


def shifted(older, newer):
    low = 0 if older is None else lax.shift_right_logical(older, 16)
    return low | jnp.left_shift(newer, 16)


def fill(table, lag, half, newer, older):
    at = pl.ds(lag * TABLE + half * HALF, HALF)
    if newer is None:
        table[at, :] = jnp.zeros((HALF, BLOCK), jnp.int32)
    elif lag % 2:
        table[at, :] = shifted(None if older is None else older[...], newer[...])
    else:
        table[at, :] = newer[...]


def arrivals(plan_ref, kind, table, w_ref):
    table[pl.ds(NDELAY * TABLE, 8), :] = jnp.zeros((8, BLOCK), jnp.int32)
    shift = row_ids(32)

    def group(i, acc):
        left, right = [], []
        for k in range(GROUP):
            code = plan_ref[kind, i * GROUP + k]
            base = jnp.right_shift(code, 7)
            slot = jnp.bitwise_and(code, SLOTS - 1)
            rows = []
            for j in range(WORDS):
                word = table[pl.ds(base + j, 1), :]
                bit = jnp.bitwise_and(jnp.right_shift(word, shift), 1)
                rows.append(bit.astype(jnp.float32).astype(jnp.bfloat16))
            left.append(jnp.concatenate(rows, axis=0))
            right.append(w_ref[pl.ds(pl.multiple_of(slot * BLOCK, BLOCK), BLOCK), :])
        left = jnp.concatenate(left, axis=1)
        right = jnp.concatenate(right, axis=0)
        return acc + jnp.dot(left, right, preferred_element_type=jnp.float32)

    zero = jnp.zeros((DMIN * TRIALS, BLOCK), jnp.float32)
    groups = (plan_ref[2, kind] + (GROUP - 1)) // GROUP
    return lax.fori_loop(0, groups, group, zero)


def early_body(n_hist):
    def body(plan_ref, *refs):
        own = list(refs[:n_hist]) + [None] * (3 - n_hist)
        other = list(refs[n_hist : 2 * n_hist - 1]) + [None] * (3 - n_hist)
        w_ref, out_ref, table = refs[2 * n_hist - 1 :]
        for lag in range(NDELAY):
            a = lag // 2
            fill(table, lag, 0, own[a], own[a + 1] if a < 2 else None)
            if lag >= 2:
                fill(table, lag, 1, other[a - 1], other[a] if a < 2 else None)
        out_ref[...] = arrivals(plan_ref, 0, table, w_ref)

    return body


def late_body(number, n_hist):
    last = number == STEPS // DMIN - 1

    def body(plan_ref, *refs):
        newer = refs[0]
        older = refs[1] if n_hist > 1 else None
        rest = refs[min(n_hist, 2) :]
        w_ref, early_ref, v_ref, drive_ref, leak_ref = rest[:5]
        count_ref = rest[5] if number else None
        v_out, pk_out, count_out, table = rest[-4:]

        for lag in range(2):
            fill(table, lag, 1, newer, older)
        current = early_ref[...] + arrivals(plan_ref, 1, table, w_ref)

        v = v_ref[...]
        if number == 0:
            v = jnp.floor(v)
        drive = drive_ref[...].astype(jnp.float32)
        leak = 1.0 / jnp.left_shift(jnp.ones((1, BLOCK), jnp.int32), leak_ref[...]).astype(jnp.float32)
        spikes = []
        for step in range(DMIN):
            arrived = jnp.concatenate(
                [current[32 * j + 16 * step : 32 * j + 16 * step + 16] for j in range(WORDS)], axis=0
            )
            v = v - jnp.floor(v * leak) + arrived + drive
            fired = v >= THRESHOLD
            v = jnp.where(fired, 0.0, jnp.maximum(v, -THRESHOLD))
            spikes.append(fired)
        v_out[...] = v
        if not last:
            store_copies(pk_out, words_of(spikes))
        counts = count_ref[...] if number else jnp.zeros((16, BLOCK), jnp.float32)
        row = row_ids(16)
        for step in range(DMIN):
            total = jnp.sum(spikes[step].astype(jnp.float32), axis=0, keepdims=True)
            counts = jnp.where(row == number * DMIN + step, total, counts)
        count_out[...] = counts
        if last:
            total = jnp.sum(counts, axis=1, keepdims=True)
            total = jnp.where(row == lane_ids(16), total, 0.0)
            total = jnp.sum(total, axis=0, keepdims=True)
            total = jnp.broadcast_to(total, (8, BLOCK))
            for copy in range(pk_out.shape[0] // 8):
                pk_out[pl.ds(8 * copy, 8), :] = total

    return body


def rates_body(counts_ref, area_ref, out_ref):
    counts = counts_ref[...]
    blocks = counts.shape[0]
    table = (area_ref[...] == row_ids(BLOCK, blocks)).astype(jnp.float32)
    sizes = jnp.sum(table, axis=1, keepdims=True) * float(TRIALS * BLOCK)
    table = table.astype(jnp.bfloat16)
    high = jnp.floor(counts * (1.0 / 128.0))
    low = counts - high * 128.0
    sums = [
        jnp.dot(table, part.astype(jnp.bfloat16), preferred_element_type=jnp.float32)
        for part in (high, low)
    ]
    rates = (sums[0] * 128.0 + sums[1]) / sizes
    out_ref[...] = jnp.transpose(rates)[:STEPS, :AREAS]


def exchanged(copies, axes):
    rows = copies.shape[0]
    peers = lax.axis_size(axes)
    pieces = copies.reshape(peers, 1, rows // peers * BLOCK)
    return lax.all_to_all(pieces, axes, split_axis=0, concat_axis=0).reshape(rows, BLOCK)


def on_device(
    initial_bits, membrane, drive, leak_shift, weights, pre_block, block_mask, delay, area_of_block
):
    words = jax.ShapeDtypeStruct((HALF, BLOCK), jnp.int32)
    volts = jax.ShapeDtypeStruct((TRIALS, BLOCK), jnp.float32)
    totals = jax.ShapeDtypeStruct((16, BLOCK), jnp.float32)
    sums = jax.ShapeDtypeStruct((DMIN * TRIALS, BLOCK), jnp.float32)
    blocks = area_of_block.shape[0]
    table = pltpu.VMEM((NDELAY * TABLE + 8, BLOCK), jnp.int32)
    ranks = lax.axis_size("rank")
    core = lax.axis_index("area_2").astype(jnp.int32).reshape(1, 1)

    flat = weights.reshape(SLOTS * BLOCK, BLOCK)
    drive = drive.reshape(1, BLOCK)
    leak_shift = leak_shift.reshape(1, BLOCK)
    v = membrane
    counts = []
    bits = jnp.transpose(initial_bits, (0, 2, 1))
    copies = kernel_call(first_body, words, [VMEM], [], "first", 8)(bits)
    plan = None
    own, other = [], []
    for number in range(STEPS // DMIN):
        mine = exchanged(copies, PLANE)
        theirs = lax.ppermute(mine, "area_2", [(0, 1), (1, 0)])
        if plan is None:
            plan = kernel_call(
                lambda *refs: plan_body(ranks, *refs),
                jax.ShapeDtypeStruct((8, SLOTS), jnp.int32),
                [SMEM, VMEM, VMEM, VMEM, ANY],
                [],
                "plan",
                8,
            )(core, pre_block, block_mask, delay, mine)
        own = [mine] + own[:2]
        n_hist = len(own)
        early = kernel_call(
            early_body(n_hist), sums, [SMEM] + [VMEM] * (2 * n_hist), [table], "early", 24
        )(plan, *own, *other[: n_hist - 1], flat)
        other = [theirs] + other[:2]
        last = number == STEPS // DMIN - 1
        out = jax.ShapeDtypeStruct((blocks, BLOCK), jnp.float32) if last else words
        rest = [*other[:2], flat, early, v, drive, leak_shift, *counts]
        v, copies, count = kernel_call(
            late_body(number, n_hist),
            (volts, out, totals),
            [SMEM] + [VMEM] * len(rest),
            [table],
            "late",
            24,
        )(plan, *rest)
        counts = [count]
    everyone = exchanged(copies, AREA_RANK)
    rates = jax.ShapeDtypeStruct((STEPS, AREAS), jnp.float32)
    rates = kernel_call(rates_body, rates, [VMEM, VMEM], [], "rates", 8)(
        everyone, area_of_block.reshape(1, blocks)
    )
    return v, rates


def solution(mesh):
    split = Mesh(
        mesh.devices.reshape(4, 4, 2, mesh.shape["rank"]), ("area_0", "area_1", "area_2", "rank")
    )
    return jax.shard_map(
        on_device,
        mesh=split,
        in_specs=(
            P(None, None, AREA_RANK),
            P(None, AREA_RANK),
            P(AREA_RANK),
            P(AREA_RANK),
            P(AREA_RANK, None, None, None),
            P(AREA_RANK, None),
            P(AREA_RANK, None),
            P(AREA_RANK, None),
            P(),
        ),
        out_specs=(P(None, AREA_RANK), P()),
        check_vma=False,
    )
```

```python
import jax
import jax.numpy as jnp
from jax import lax
from jax.experimental import pallas as pl
from jax.experimental.pallas import tpu as pltpu
from jax.sharding import Mesh
from jax.sharding import PartitionSpec as P

AREAS = 32
DMIN = 2
NDELAY = 4
STEPS = 10
BLOCK = 128
TRIALS = 48
SLOTS = 128
THRESHOLD = 200.0
GROUP = 16
WORDS = 3
HALF = 128 * WORDS
TABLE = 2 * HALF
AREA_RANK = ("area_0", "area_1", "area_2", "rank")
PLANE = ("area_0", "area_1", "rank")

VMEM = pl.BlockSpec(memory_space=pltpu.VMEM)
SMEM = pl.BlockSpec(memory_space=pltpu.SMEM)


def kernel_call(body, outs, ins, scratch, name, limit, cost=None):
    return pl.pallas_call(
        body,
        out_shape=outs,
        in_specs=ins,
        out_specs=jax.tree.map(lambda _: VMEM, outs),
        scratch_shapes=scratch,
        name=name,
        cost_estimate=cost,
        compiler_params=pltpu.CompilerParams(vmem_limit_bytes=limit << 20),
    )


def row_ids(rows, lanes=BLOCK):
    return lax.broadcasted_iota(jnp.int32, (rows, lanes), 0)


def lane_ids(rows, lanes=BLOCK):
    return lax.broadcasted_iota(jnp.int32, (rows, lanes), 1)


def words_of(spikes):
    words = []
    for j in range(WORDS):
        bits = jnp.zeros((8, BLOCK), jnp.int32)
        for step in range(DMIN):
            for part in range(2):
                shift = row_ids(8) + (8 * part + 16 * step)
                flags = spikes[step][16 * j + 8 * part : 16 * j + 8 * part + 8]
                bits = bits | jnp.where(flags, jnp.left_shift(1, shift), 0)
        words.append(jnp.sum(bits, axis=0, keepdims=True, dtype=jnp.int32))
    return words


def store_copies(out_ref, words):
    which = row_ids(24) % WORDS
    rows = jnp.where(which == 0, words[0], jnp.where(which == 1, words[1], words[2]))
    for copy in range(HALF // 24):
        out_ref[pl.ds(24 * copy, 24), :] = rows


def first_body(input_ref, out_ref, early_ref, late_ref):
    trial = lane_ids(8, TRIALS)
    which = row_ids(8, TRIALS)
    place = jnp.left_shift(1, trial % 16).astype(jnp.float32)
    places = jnp.where(trial // 16 == which, place, 0.0).astype(jnp.bfloat16)
    packed = jnp.zeros((8, BLOCK), jnp.int32)
    shift = row_ids(32, TRIALS)
    for step in range(DMIN):
        bits = [
            jnp.bitwise_and(jnp.right_shift(input_ref[4 * step + w : 4 * step + w + 1, :TRIALS], shift), 1)
            for w in range(BLOCK // 32)
        ]
        bits = jnp.concatenate(bits, axis=0).astype(jnp.float32).astype(jnp.bfloat16)
        half = lax.dot_general(
            places, bits, (((1,), (1,)), ((), ())), preferred_element_type=jnp.float32
        )
        packed = packed | jnp.left_shift(half.astype(jnp.int32), 16 * step)
    store_copies(out_ref, [packed[j : j + 1] for j in range(WORDS)])
    rows = [input_ref[8 + i : 9 + i, :] for i in range(4)]
    plan(slot_codes(lax.axis_size("rank"), *rows), (early_ref, late_ref))


def slot_codes(ranks, pre, mask, delay, core):
    lag = delay - DMIN
    other = jnp.bitwise_xor(pre // ranks % 2, core)
    place = pre // (2 * ranks) * ranks + pre % ranks
    base = lag * TABLE + other * HALF + place * WORDS
    late = jnp.where((other == 1) & (lag < 2), 1, 0)
    kind = jnp.where(mask == 1, late, 2)
    return kind * (1 << 20) + base * SLOTS + lane_ids(1)


def plan(slots, out_refs):
    kind = jnp.right_shift(slots, 20)
    code = jnp.bitwise_and(slots, (1 << 20) - 1)

    def column(row):
        return jnp.transpose(jnp.broadcast_to(row, (SLOTS, SLOTS)))

    sub, lane = row_ids(SLOTS), lane_ids(SLOTS)
    kind_col, code_col = column(kind), column(code)
    kind_row = jnp.broadcast_to(kind, (SLOTS, SLOTS))
    before = jnp.where((kind_row == kind_col) & (lane < sub), 1, 0)
    rank_col = jnp.sum(before, axis=1, keepdims=True, dtype=jnp.int32)
    nothing = NDELAY * TABLE * SLOTS
    for k in range(2):
        hit = (kind_col == k) & (rank_col == lane)
        codes = jnp.sum(jnp.where(hit, code_col - nothing, 0), axis=0, keepdims=True, dtype=jnp.int32)
        count = jnp.sum(jnp.where(kind == k, 1, 0), axis=1, keepdims=True, dtype=jnp.int32)
        codes = codes + nothing + jnp.where(lane_ids(1) == 0, jnp.left_shift(count, 20), 0)
        out_refs[k][...] = codes


def shifted(older, newer):
    low = 0 if older is None else lax.shift_right_logical(older, 16)
    return low | jnp.left_shift(newer, 16)


def fill(table, lag, half, newer, older):
    at = pl.ds(lag * TABLE + half * HALF, HALF)
    if newer is None:
        table[at, :] = jnp.zeros((HALF, BLOCK), jnp.int32)
    elif lag % 2:
        table[at, :] = shifted(None if older is None else older[...], newer[...])
    else:
        table[at, :] = newer[...]


def arrivals(plan_ref, table, w_ref):
    table[pl.ds(NDELAY * TABLE, 8), :] = jnp.zeros((8, BLOCK), jnp.int32)
    mask = jnp.left_shift(1, row_ids(32))

    def group(i, acc):
        left, right = [], []
        for k in range(GROUP):
            code = plan_ref[0, i * GROUP + k]
            base = jnp.bitwise_and(jnp.right_shift(code, 7), (1 << 13) - 1)
            slot = jnp.bitwise_and(code, SLOTS - 1)
            rows = []
            for j in range(WORDS):
                word = table[pl.ds(base + j, 1), :]
                bit = jnp.bitwise_and(word, mask)
                rows.append(bit.astype(jnp.float32).astype(jnp.bfloat16))
            left.append(jnp.concatenate(rows, axis=0))
            right.append(w_ref[pl.ds(pl.multiple_of(slot * BLOCK, BLOCK), BLOCK), :])
        left = jnp.concatenate(left, axis=1)
        right = jnp.concatenate(right, axis=0)
        return acc + jnp.dot(left, right, preferred_element_type=jnp.float32)

    zero = jnp.zeros((DMIN * TRIALS, BLOCK), jnp.float32)
    groups = jnp.right_shift(jnp.right_shift(plan_ref[0, 0], 20) + (GROUP - 1), 4)
    return lax.fori_loop(0, groups, group, zero)


def early_body(n_hist):
    def body(plan_ref, *refs):
        own = list(refs[:n_hist]) + [None] * (3 - n_hist)
        other = list(refs[n_hist : 2 * n_hist - 1]) + [None] * (3 - n_hist)
        w_ref, out_ref, table = refs[2 * n_hist - 1 :]
        for lag in range(NDELAY):
            a = lag // 2
            fill(table, lag, 0, own[a], own[a + 1] if a < 2 else None)
            if lag >= 2:
                fill(table, lag, 1, other[a - 1], other[a] if a < 2 else None)
        out_ref[...] = arrivals(plan_ref, table, w_ref)

    return body


def late_body(number, n_hist):
    last = number == STEPS // DMIN - 1

    def body(plan_ref, *refs):
        newer = refs[0]
        older = refs[1] if n_hist > 1 else None
        rest = refs[min(n_hist, 2) :]
        w_ref, early_ref, v_ref, drive_ref, leak_ref = rest[:5]
        count_ref = rest[5] if number else None
        v_out, pk_out, count_out, table = rest[-4:]

        for lag in range(2):
            fill(table, lag, 1, newer, older)
        current = early_ref[...] + arrivals(plan_ref, table, w_ref)
        bit = row_ids(32)
        power = jnp.left_shift(1, jnp.maximum(30 - bit, 0)).astype(jnp.float32)
        scale = jnp.where(bit == 31, -(2.0**-31), power * 2.0**-30)

        v = v_ref[...]
        if number == 0:
            v = jnp.floor(v)
        drive = drive_ref[...].astype(jnp.float32)
        leak = 1.0 / jnp.left_shift(jnp.ones((1, BLOCK), jnp.int32), leak_ref[...]).astype(jnp.float32)
        spikes = []
        for step in range(DMIN):
            arrived = jnp.concatenate(
                [
                    current[32 * j + 16 * step : 32 * j + 16 * step + 16]
                    * scale[16 * step : 16 * step + 16]
                    for j in range(WORDS)
                ],
                axis=0,
            )
            v = v - jnp.floor(v * leak) + arrived + drive
            fired = v >= THRESHOLD
            v = jnp.where(fired, 0.0, jnp.maximum(v, -THRESHOLD))
            spikes.append(fired)
        v_out[...] = v
        if not last:
            store_copies(pk_out, words_of(spikes))
        counts = count_ref[...] if number else jnp.zeros((16, BLOCK), jnp.float32)
        row = row_ids(16)
        for step in range(DMIN):
            total = jnp.sum(spikes[step].astype(jnp.float32), axis=0, keepdims=True)
            counts = jnp.where(row == number * DMIN + step, total, counts)
        count_out[...] = counts
        if last:
            total = jnp.sum(counts, axis=1, keepdims=True)
            total = jnp.where(row == lane_ids(16), total, 0.0)
            total = jnp.sum(total, axis=0, keepdims=True)
            total = jnp.broadcast_to(total, (8, BLOCK))
            for copy in range(pk_out.shape[0] // 8):
                pk_out[pl.ds(8 * copy, 8), :] = total

    return body


def rates_body(counts_ref, area_ref, v_ref, out_ref, v_out):
    v_out[...] = v_ref[...]
    counts = counts_ref[...]
    blocks = counts.shape[0]
    table = (area_ref[...] == row_ids(BLOCK, blocks)).astype(jnp.float32)
    sizes = jnp.sum(table, axis=1, keepdims=True) * float(TRIALS * BLOCK)
    table = table.astype(jnp.bfloat16)
    high = jnp.floor(counts * (1.0 / 128.0))
    low = counts - high * 128.0
    sums = [
        jnp.dot(table, part.astype(jnp.bfloat16), preferred_element_type=jnp.float32)
        for part in (high, low)
    ]
    rates = (sums[0] * 128.0 + sums[1]) / sizes
    out_ref[...] = jnp.transpose(rates)[:STEPS, :AREAS]


def exchanged(copies, axes):
    rows = copies.shape[0]
    peers = lax.axis_size(axes)
    pieces = copies.reshape(peers, 1, rows // peers * BLOCK)
    return lax.all_to_all(pieces, axes, split_axis=0, concat_axis=0).reshape(rows, BLOCK)


def on_device(
    initial_bits, membrane, drive, leak_shift, weights, pre_block, block_mask, delay, area_of_block
):
    words = jax.ShapeDtypeStruct((HALF, BLOCK), jnp.int32)
    volts = jax.ShapeDtypeStruct((TRIALS, BLOCK), jnp.float32)
    totals = jax.ShapeDtypeStruct((16, BLOCK), jnp.float32)
    sums = jax.ShapeDtypeStruct((DMIN * TRIALS, BLOCK), jnp.float32)
    blocks = area_of_block.shape[0]
    table = pltpu.VMEM((NDELAY * TABLE + 8, BLOCK), jnp.int32)
    codes = jax.ShapeDtypeStruct((1, SLOTS), jnp.int32)

    flat = weights.reshape(SLOTS * BLOCK, BLOCK)
    drive = drive.reshape(1, BLOCK)
    leak_shift = leak_shift.reshape(1, BLOCK)
    v = membrane
    counts = []
    bits = jnp.transpose(initial_bits, (0, 2, 1)).reshape(8, TRIALS)
    first_input = jnp.pad(bits, ((0, 8), (0, BLOCK - TRIALS)))
    core = lax.broadcast(lax.axis_index("area_2"), (1, BLOCK))
    for row, values in enumerate((pre_block, block_mask, delay, core), 8):
        first_input = jnp.where(row_ids(16) == row, values, first_input)
    copies, early_plan, late_plan = kernel_call(
        first_body,
        (words, codes, codes),
        [VMEM],
        [],
        "first",
        8,
        pl.CostEstimate(flops=10**10, bytes_accessed=1 << 18, transcendentals=0),
    )(first_input)
    own, other = [], []
    for number in range(STEPS // DMIN):
        mine = exchanged(copies, PLANE)
        theirs = lax.ppermute(mine, "area_2", [(0, 1), (1, 0)])
        own = [mine] + own[:2]
        n_hist = len(own)
        early = kernel_call(
            early_body(n_hist), sums, [SMEM] + [VMEM] * (2 * n_hist), [table], "early", 24
        )(early_plan, *own, *other[: n_hist - 1], flat)
        other = [theirs] + other[:2]
        last = number == STEPS // DMIN - 1
        out = jax.ShapeDtypeStruct((blocks, BLOCK), jnp.float32) if last else words
        rest = [*other[:2], flat, early, v, drive, leak_shift, *counts]
        v, copies, count = kernel_call(
            late_body(number, n_hist),
            (volts, out, totals),
            [SMEM] + [VMEM] * len(rest),
            [table],
            "late",
            24,
        )(late_plan, *rest)
        counts = [count]
    everyone = exchanged(copies, AREA_RANK)
    rates = jax.ShapeDtypeStruct((STEPS, AREAS), jnp.float32)
    rates, v = kernel_call(rates_body, (rates, volts), [VMEM] * 3, [], "rates", 8)(
        everyone, area_of_block.reshape(1, blocks), v
    )
    return v, rates


def solution(mesh):
    split = Mesh(
        mesh.devices.reshape(4, 4, 2, mesh.shape["rank"]), ("area_0", "area_1", "area_2", "rank")
    )
    return jax.shard_map(
        on_device,
        mesh=split,
        in_specs=(
            P(None, None, AREA_RANK),
            P(None, AREA_RANK),
            P(AREA_RANK),
            P(AREA_RANK),
            P(AREA_RANK, None, None, None),
            P(AREA_RANK, None),
            P(AREA_RANK, None),
            P(AREA_RANK, None),
            P(),
        ),
        out_specs=(P(None, AREA_RANK), P()),
        check_vma=False,
    )
```

```python
import jax
import jax.numpy as jnp
from jax import lax
from jax.experimental import pallas as pl
from jax.experimental.pallas import tpu as pltpu
from jax.sharding import Mesh
from jax.sharding import PartitionSpec as P

AREAS = 32
DMIN = 2
NDELAY = 4
STEPS = 10
BLOCK = 128
TRIALS = 48
SLOTS = 128
THRESHOLD = 200.0
GROUP = 48
PLAN = 144
WORDS = 3
HALF = 128 * WORDS
TABLE = 2 * HALF
AREA_RANK = ("area_0", "area_1", "area_2", "rank")
PLANE = ("area_0", "area_1", "rank")

VMEM = pl.BlockSpec(memory_space=pltpu.VMEM)


def kernel_call(body, outs, ins, scratch, name, limit, cost=None):
    return pl.pallas_call(
        body,
        out_shape=outs,
        in_specs=ins,
        out_specs=jax.tree.map(lambda _: VMEM, outs),
        scratch_shapes=scratch,
        name=name,
        cost_estimate=cost,
        compiler_params=pltpu.CompilerParams(vmem_limit_bytes=limit << 20),
    )


def row_ids(rows, lanes=BLOCK):
    return lax.broadcasted_iota(jnp.int32, (rows, lanes), 0)


def lane_ids(rows, lanes=BLOCK):
    return lax.broadcasted_iota(jnp.int32, (rows, lanes), 1)


def words_of(spikes):
    words = []
    for j in range(WORDS):
        bits = jnp.zeros((8, BLOCK), jnp.int32)
        for step in range(DMIN):
            for part in range(2):
                shift = row_ids(8) + (8 * part + 16 * step)
                flags = spikes[step][16 * j + 8 * part : 16 * j + 8 * part + 8]
                bits = bits | jnp.where(flags, jnp.left_shift(1, shift), 0)
        words.append(jnp.sum(bits, axis=0, keepdims=True, dtype=jnp.int32))
    return words


def store_copies(out_ref, words):
    which = row_ids(24) % WORDS
    rows = jnp.where(which == 0, words[0], jnp.where(which == 1, words[1], words[2]))
    for copy in range(HALF // 24):
        out_ref[pl.ds(24 * copy, 24), :] = rows


def first_body(input_ref, out_ref, early_ref, late_ref):
    trial = lane_ids(8, TRIALS)
    which = row_ids(8, TRIALS)
    place = jnp.left_shift(1, trial % 16).astype(jnp.float32)
    places = jnp.where(trial // 16 == which, place, 0.0).astype(jnp.bfloat16)
    packed = jnp.zeros((8, BLOCK), jnp.int32)
    shift = row_ids(32, TRIALS)
    for step in range(DMIN):
        bits = [
            jnp.bitwise_and(jnp.right_shift(input_ref[4 * step + w : 4 * step + w + 1, :TRIALS], shift), 1)
            for w in range(BLOCK // 32)
        ]
        bits = jnp.concatenate(bits, axis=0).astype(jnp.float32).astype(jnp.bfloat16)
        half = lax.dot_general(
            places, bits, (((1,), (1,)), ((), ())), preferred_element_type=jnp.float32
        )
        packed = packed | jnp.left_shift(half.astype(jnp.int32), 16 * step)
    store_copies(out_ref, [packed[j : j + 1] for j in range(WORDS)])
    rows = [input_ref[8 + i : 9 + i, :] for i in range(4)]
    plan(slot_codes(lax.axis_size("rank"), *rows), (early_ref, late_ref))


def slot_codes(ranks, pre, mask, delay, core):
    lag = delay - DMIN
    other = jnp.bitwise_xor(pre // ranks % 2, core)
    place = pre // (2 * ranks) * ranks + pre % ranks
    base = lag * TABLE + other * HALF + place * WORDS
    late = jnp.where((other == 1) & (lag < 2), 1, 0)
    kind = jnp.where(mask == 1, late, 2)
    return kind * (1 << 20) + base * SLOTS + lane_ids(1)


def plan(slots, out_refs):
    kind = jnp.broadcast_to(jnp.right_shift(slots, 20), (SLOTS, SLOTS))
    code = jnp.bitwise_and(slots, (1 << 20) - 1)
    sub, lane = row_ids(SLOTS), lane_ids(SLOTS)
    before = jnp.where((jnp.transpose(kind) == kind) & (sub < lane), 1, 0)
    rank = jnp.sum(before, axis=0, keepdims=True, dtype=jnp.int32)
    nothing = NDELAY * TABLE * SLOTS
    for k, out_ref in enumerate(out_refs):
        hit = (kind == k) & (rank == sub)
        codes = jnp.sum(jnp.where(hit, code - nothing, 0), axis=1, keepdims=True, dtype=jnp.int32)
        count = jnp.where(kind == k, 1, 0)
        count = jnp.sum(count, axis=1, keepdims=True, dtype=jnp.int32)
        codes = codes + nothing + jnp.where(sub == 0, jnp.left_shift(count, 20), 0)
        out_ref[pl.ds(0, SLOTS), :] = codes
        out_ref[pl.ds(SLOTS, PLAN - SLOTS), :] = jnp.full((PLAN - SLOTS, SLOTS), nothing, jnp.int32)


def shifted(older, newer):
    low = 0 if older is None else lax.shift_right_logical(older, 16)
    return low | jnp.left_shift(newer, 16)


def fill(table, lag, half, newer, older):
    at = pl.ds(lag * TABLE + half * HALF, HALF)
    if newer is None:
        table[at, :] = jnp.zeros((HALF, BLOCK), jnp.int32)
    elif lag % 2:
        table[at, :] = shifted(None if older is None else older[...], newer[...])
    else:
        table[at, :] = newer[...]


def arrivals(plan_ref, table, w_ref):
    table[pl.ds(NDELAY * TABLE, 8), :] = jnp.zeros((8, BLOCK), jnp.int32)
    mask = jnp.left_shift(1, row_ids(32))

    def group(i, acc):
        left, right = [], []
        for k in range(GROUP):
            code = plan_ref[i * GROUP + k, 0]
            base = jnp.bitwise_and(jnp.right_shift(code, 7), (1 << 13) - 1)
            slot = jnp.bitwise_and(code, SLOTS - 1)
            rows = []
            for j in range(WORDS):
                word = table[pl.ds(base + j, 1), :]
                bit = jnp.bitwise_and(word, mask)
                rows.append(bit.astype(jnp.float32).astype(jnp.bfloat16))
            left.append(jnp.concatenate(rows, axis=0))
            right.append(w_ref[pl.ds(pl.multiple_of(slot * BLOCK, BLOCK), BLOCK), :])
        left = jnp.concatenate(left, axis=1)
        right = jnp.concatenate(right, axis=0)
        return acc + jnp.dot(left, right, preferred_element_type=jnp.float32)

    zero = jnp.zeros((DMIN * TRIALS, BLOCK), jnp.float32)
    count = jnp.right_shift(plan_ref[0, 0], 20)
    groups = sum((count > i).astype(jnp.int32) for i in range(0, SLOTS, GROUP))
    return lax.fori_loop(0, groups, group, zero)


def early_body(n_hist):
    def body(plan_ref, *refs):
        own = list(refs[:n_hist]) + [None] * (3 - n_hist)
        other = list(refs[n_hist : 2 * n_hist - 1]) + [None] * (3 - n_hist)
        w_ref, out_ref, table = refs[2 * n_hist - 1 :]
        for lag in range(NDELAY):
            a = lag // 2
            fill(table, lag, 0, own[a], own[a + 1] if a < 2 else None)
            if lag >= 2:
                fill(table, lag, 1, other[a - 1], other[a] if a < 2 else None)
        out_ref[...] = arrivals(plan_ref, table, w_ref)

    return body


def late_body(number, n_hist):
    last = number == STEPS // DMIN - 1

    def body(plan_ref, *refs):
        newer = refs[0]
        older = refs[1] if n_hist > 1 else None
        rest = refs[min(n_hist, 2) :]
        w_ref, early_ref, v_ref, drive_ref, leak_ref = rest[:5]
        count_ref = rest[5] if number else None
        v_out, pk_out = rest[-3 - (not last) : -1 - (not last)]
        table = rest[-1]

        for lag in range(2):
            fill(table, lag, 1, newer, older)
        current = early_ref[...] + arrivals(plan_ref, table, w_ref)
        bit = row_ids(32)
        power = jnp.left_shift(1, jnp.maximum(30 - bit, 0)).astype(jnp.float32)
        scale = jnp.where(bit == 31, -(2.0**-31), power * 2.0**-30)

        v = v_ref[...]
        if number == 0:
            v = jnp.floor(v)
        drive = drive_ref[...].astype(jnp.float32)
        leak = 1.0 / jnp.left_shift(jnp.ones((1, BLOCK), jnp.int32), leak_ref[...]).astype(jnp.float32)
        spikes = []
        for step in range(DMIN):
            arrived = jnp.concatenate(
                [
                    current[32 * j + 16 * step : 32 * j + 16 * step + 16]
                    * scale[16 * step : 16 * step + 16]
                    for j in range(WORDS)
                ],
                axis=0,
            )
            v = v - jnp.floor(v * leak) + arrived + drive
            fired = v >= THRESHOLD
            v = jnp.where(fired, 0.0, jnp.maximum(v, -THRESHOLD))
            spikes.append(fired)
        v_out[...] = v
        if not last:
            store_copies(pk_out, words_of(spikes))
        counts = count_ref[...] if number else jnp.zeros((16, BLOCK), jnp.float32)
        row = row_ids(16)
        for step in range(DMIN):
            total = jnp.sum(spikes[step].astype(jnp.float32), axis=0, keepdims=True)
            counts = jnp.where(row == number * DMIN + step, total, counts)
        if not last:
            rest[-2][...] = counts
        else:
            total = jnp.sum(counts, axis=1, keepdims=True)
            total = jnp.where(row == lane_ids(16), total, 0.0)
            total = jnp.sum(total, axis=0, keepdims=True)
            total = jnp.broadcast_to(total, (8, BLOCK))
            for copy in range(pk_out.shape[0] // 8):
                pk_out[pl.ds(8 * copy, 8), :] = total

    return body


def rates_body(counts_ref, area_ref, v_ref, out_ref, v_out):
    v_out[...] = v_ref[...]
    counts = counts_ref[...]
    blocks = counts.shape[0]
    table = (area_ref[...] == row_ids(BLOCK, blocks)).astype(jnp.float32)
    sizes = jnp.sum(table, axis=1, keepdims=True) * float(TRIALS * BLOCK)
    table = table.astype(jnp.bfloat16)
    high = jnp.floor(counts * (1.0 / 128.0))
    low = counts - high * 128.0
    sums = [
        jnp.dot(table, part.astype(jnp.bfloat16), preferred_element_type=jnp.float32)
        for part in (high, low)
    ]
    rates = (sums[0] * 128.0 + sums[1]) / sizes
    out_ref[...] = jnp.transpose(rates)[:STEPS, :AREAS]


def exchanged(copies, axes):
    rows = copies.shape[0]
    peers = lax.axis_size(axes)
    pieces = copies.reshape(peers, 1, rows // peers * BLOCK)
    return lax.all_to_all(pieces, axes, split_axis=0, concat_axis=0).reshape(rows, BLOCK)


def on_device(
    initial_bits, membrane, drive, leak_shift, weights, pre_block, block_mask, delay, area_of_block
):
    words = jax.ShapeDtypeStruct((HALF, BLOCK), jnp.int32)
    volts = jax.ShapeDtypeStruct((TRIALS, BLOCK), jnp.float32)
    totals = jax.ShapeDtypeStruct((16, BLOCK), jnp.float32)
    sums = jax.ShapeDtypeStruct((DMIN * TRIALS, BLOCK), jnp.float32)
    blocks = area_of_block.shape[0]
    table = pltpu.VMEM((NDELAY * TABLE + 8, BLOCK), jnp.int32)
    codes = jax.ShapeDtypeStruct((PLAN, SLOTS), jnp.int32)

    flat = weights.reshape(SLOTS * BLOCK, BLOCK)
    drive = drive.reshape(1, BLOCK)
    leak_shift = leak_shift.reshape(1, BLOCK)
    v = membrane
    counts = []
    bits = jnp.transpose(initial_bits, (0, 2, 1)).reshape(8, TRIALS)
    first_input = jnp.pad(bits, ((0, 8), (0, BLOCK - TRIALS)))
    core = lax.broadcast(lax.axis_index("area_2"), (1, BLOCK))
    for row, values in enumerate((pre_block, block_mask, delay, core), 8):
        first_input = jnp.where(row_ids(16) == row, values, first_input)
    copies, early_plan, late_plan = kernel_call(
        first_body,
        (words, codes, codes),
        [VMEM],
        [],
        "first",
        8,
        pl.CostEstimate(flops=10**10, bytes_accessed=1 << 18, transcendentals=0),
    )(first_input)
    own, other = [], []
    for number in range(STEPS // DMIN):
        mine = exchanged(copies, PLANE)
        theirs = lax.ppermute(mine, "area_2", [(0, 1), (1, 0)])
        own = [mine] + own[:2]
        n_hist = len(own)
        early = kernel_call(
            early_body(n_hist), sums, [VMEM] + [VMEM] * (2 * n_hist), [table], "early", 24
        )(early_plan, *own, *other[: n_hist - 1], flat)
        other = [theirs] + other[:2]
        last = number == STEPS // DMIN - 1
        out = jax.ShapeDtypeStruct((blocks, BLOCK), jnp.float32) if last else words
        rest = [*other[:2], flat, early, v, drive, leak_shift, *counts]
        v, copies, *counts = kernel_call(
            late_body(number, n_hist),
            (volts, out) if last else (volts, out, totals),
            [VMEM] + [VMEM] * len(rest),
            [table],
            "late",
            24,
        )(late_plan, *rest)
    everyone = exchanged(copies, AREA_RANK)
    rates = jax.ShapeDtypeStruct((STEPS, AREAS), jnp.float32)
    rates, v = kernel_call(rates_body, (rates, volts), [VMEM] * 3, [], "rates", 8)(
        everyone, area_of_block.reshape(1, blocks), v
    )
    return v, rates


def solution(mesh):
    split = Mesh(
        mesh.devices.reshape(4, 4, 2, mesh.shape["rank"]), ("area_0", "area_1", "area_2", "rank")
    )
    return jax.shard_map(
        on_device,
        mesh=split,
        in_specs=(
            P(None, None, AREA_RANK),
            P(None, AREA_RANK),
            P(AREA_RANK),
            P(AREA_RANK),
            P(AREA_RANK, None, None, None),
            P(AREA_RANK, None),
            P(AREA_RANK, None),
            P(AREA_RANK, None),
            P(),
        ),
        out_specs=(P(None, AREA_RANK), P()),
        check_vma=False,
    )
```

```python
import jax
import jax.numpy as jnp
from jax import lax
from jax.experimental import pallas as pl
from jax.experimental.pallas import tpu as pltpu
from jax.sharding import Mesh
from jax.sharding import PartitionSpec as P

AREAS = 32
DMIN = 2
NDELAY = 4
STEPS = 10
BLOCK = 128
TRIALS = 48
SLOTS = 128
THRESHOLD = 200.0
GROUP = 48
PLAN = 144
WORDS = 3
HALF = 128 * WORDS
TABLE = 2 * HALF
CHIPS = (4, 4, 8)
CORE = 8

VMEM = pl.BlockSpec(memory_space=pltpu.VMEM)


def kernel_call(body, outs, ins, scratch, name, limit, cost=None):
    return pl.pallas_call(
        body,
        out_shape=outs,
        in_specs=ins,
        out_specs=jax.tree.map(lambda _: VMEM, outs),
        scratch_shapes=scratch,
        name=name,
        cost_estimate=cost,
        compiler_params=pltpu.CompilerParams(vmem_limit_bytes=limit << 20),
    )


def row_ids(rows, lanes=BLOCK):
    return lax.broadcasted_iota(jnp.int32, (rows, lanes), 0)


def lane_ids(rows, lanes=BLOCK):
    return lax.broadcasted_iota(jnp.int32, (rows, lanes), 1)


def words_of(spikes):
    words = []
    for j in range(WORDS):
        bits = jnp.zeros((8, BLOCK), jnp.int32)
        for step in range(DMIN):
            for part in range(2):
                shift = row_ids(8) + (8 * part + 16 * step)
                flags = spikes[step][16 * j + 8 * part : 16 * j + 8 * part + 8]
                bits = bits | jnp.where(flags, jnp.left_shift(1, shift), 0)
        words.append(jnp.sum(bits, axis=0, keepdims=True, dtype=jnp.int32))
    return words


def store_copies(out_ref, words):
    which = row_ids(24) % WORDS
    rows = jnp.where(which == 0, words[0], jnp.where(which == 1, words[1], words[2]))
    for copy in range(HALF // 24):
        out_ref[pl.ds(24 * copy, 24), :] = rows


def first_body(input_ref, out_ref, early_ref, late_ref):
    trial = lane_ids(8, TRIALS)
    which = row_ids(8, TRIALS)
    place = jnp.left_shift(1, trial % 16).astype(jnp.float32)
    places = jnp.where(trial // 16 == which, place, 0.0).astype(jnp.bfloat16)
    packed = jnp.zeros((8, BLOCK), jnp.int32)
    shift = row_ids(32, TRIALS)
    for step in range(DMIN):
        bits = [
            jnp.bitwise_and(jnp.right_shift(input_ref[4 * step + w : 4 * step + w + 1, :TRIALS], shift), 1)
            for w in range(BLOCK // 32)
        ]
        bits = jnp.concatenate(bits, axis=0).astype(jnp.float32).astype(jnp.bfloat16)
        half = lax.dot_general(
            places, bits, (((1,), (1,)), ((), ())), preferred_element_type=jnp.float32
        )
        packed = packed | jnp.left_shift(half.astype(jnp.int32), 16 * step)
    store_copies(out_ref, [packed[j : j + 1] for j in range(WORDS)])
    rows = [input_ref[8 + i : 9 + i, :] for i in range(4)]
    plan(slot_codes(*rows), (early_ref, late_ref))


def chip_order(block):
    y, x, z = block // 64, block // 16 % 4, block % 8
    return (x * CHIPS[2] + z) * CHIPS[0] + y


def slot_codes(pre, mask, delay, device):
    lag = delay - DMIN
    other = jnp.bitwise_and(jnp.bitwise_xor(pre, device), CORE) // CORE
    place = chip_order(pre)
    base = lag * TABLE + other * HALF + place * WORDS
    late = jnp.where((other == 1) & (lag < 2), 1, 0)
    kind = jnp.where(mask == 1, late, 2)
    return kind * (1 << 20) + base * SLOTS + lane_ids(1)


def plan(slots, out_refs):
    kind = jnp.broadcast_to(jnp.right_shift(slots, 20), (SLOTS, SLOTS))
    code = jnp.bitwise_and(slots, (1 << 20) - 1)
    sub, lane = row_ids(SLOTS), lane_ids(SLOTS)
    before = jnp.where((jnp.transpose(kind) == kind) & (sub < lane), 1, 0)
    rank = jnp.sum(before, axis=0, keepdims=True, dtype=jnp.int32)
    nothing = NDELAY * TABLE * SLOTS
    for k, out_ref in enumerate(out_refs):
        hit = (kind == k) & (rank == sub)
        codes = jnp.sum(jnp.where(hit, code - nothing, 0), axis=1, keepdims=True, dtype=jnp.int32)
        count = jnp.where(kind == k, 1, 0)
        count = jnp.sum(count, axis=1, keepdims=True, dtype=jnp.int32)
        codes = codes + nothing + jnp.where(sub == 0, jnp.left_shift(count, 20), 0)
        out_ref[pl.ds(0, SLOTS), :] = codes
        out_ref[pl.ds(SLOTS, PLAN - SLOTS), :] = jnp.full((PLAN - SLOTS, SLOTS), nothing, jnp.int32)


def shifted(older, newer):
    low = 0 if older is None else lax.shift_right_logical(older, 16)
    return low | jnp.left_shift(newer, 16)


def fill(table, lag, half, newer, older):
    at = pl.ds(lag * TABLE + half * HALF, HALF)
    if newer is None:
        table[at, :] = jnp.zeros((HALF, BLOCK), jnp.int32)
    elif lag % 2:
        table[at, :] = shifted(None if older is None else older[...], newer[...])
    else:
        table[at, :] = newer[...]


def arrivals(plan_ref, table, w_ref):
    table[pl.ds(NDELAY * TABLE, 8), :] = jnp.zeros((8, BLOCK), jnp.int32)
    mask = jnp.left_shift(1, row_ids(32))

    def group(i, acc):
        left, right = [], []
        for k in range(GROUP):
            code = plan_ref[i * GROUP + k, 0]
            base = jnp.bitwise_and(jnp.right_shift(code, 7), (1 << 13) - 1)
            slot = jnp.bitwise_and(code, SLOTS - 1)
            rows = []
            for j in range(WORDS):
                word = table[pl.ds(base + j, 1), :]
                bit = jnp.bitwise_and(word, mask)
                rows.append(bit.astype(jnp.float32).astype(jnp.bfloat16))
            left.append(jnp.concatenate(rows, axis=0))
            right.append(w_ref[pl.ds(pl.multiple_of(slot * BLOCK, BLOCK), BLOCK), :])
        left = jnp.concatenate(left, axis=1)
        right = jnp.concatenate(right, axis=0)
        return acc + jnp.dot(left, right, preferred_element_type=jnp.float32)

    zero = jnp.zeros((DMIN * TRIALS, BLOCK), jnp.float32)
    count = jnp.right_shift(plan_ref[0, 0], 20)
    groups = sum((count > i).astype(jnp.int32) for i in range(0, SLOTS, GROUP))
    return lax.fori_loop(0, groups, group, zero)


def early_body(n_hist):
    def body(plan_ref, *refs):
        own = list(refs[:n_hist]) + [None] * (3 - n_hist)
        other = list(refs[n_hist : 2 * n_hist - 1]) + [None] * (3 - n_hist)
        w_ref, out_ref, table = refs[2 * n_hist - 1 :]
        for lag in range(NDELAY):
            a = lag // 2
            fill(table, lag, 0, own[a], own[a + 1] if a < 2 else None)
            if lag >= 2:
                fill(table, lag, 1, other[a - 1], other[a] if a < 2 else None)
        out_ref[...] = arrivals(plan_ref, table, w_ref)

    return body


def late_body(number, n_hist):
    last = number == STEPS // DMIN - 1

    def body(plan_ref, *refs):
        newer = refs[0]
        older = refs[1] if n_hist > 1 else None
        rest = refs[min(n_hist, 2) :]
        w_ref, early_ref, v_ref, drive_ref, leak_ref = rest[:5]
        count_ref = rest[5] if number else None
        v_out, pk_out = rest[-3 - (not last) : -1 - (not last)]
        table = rest[-1]

        for lag in range(2):
            fill(table, lag, 1, newer, older)
        current = early_ref[...] + arrivals(plan_ref, table, w_ref)
        bit = row_ids(32)
        power = jnp.left_shift(1, jnp.maximum(30 - bit, 0)).astype(jnp.float32)
        scale = jnp.where(bit == 31, -(2.0**-31), power * 2.0**-30)

        v = v_ref[...]
        if number == 0:
            v = jnp.floor(v)
        drive = drive_ref[...].astype(jnp.float32)
        leak = 1.0 / jnp.left_shift(jnp.ones((1, BLOCK), jnp.int32), leak_ref[...]).astype(jnp.float32)
        spikes = []
        for step in range(DMIN):
            arrived = jnp.concatenate(
                [
                    current[32 * j + 16 * step : 32 * j + 16 * step + 16]
                    * scale[16 * step : 16 * step + 16]
                    for j in range(WORDS)
                ],
                axis=0,
            )
            v = v - jnp.floor(v * leak) + arrived + drive
            fired = v >= THRESHOLD
            v = jnp.where(fired, 0.0, jnp.maximum(v, -THRESHOLD))
            spikes.append(fired)
        v_out[...] = v
        if not last:
            store_copies(pk_out, words_of(spikes))
        counts = count_ref[...] if number else jnp.zeros((16, BLOCK), jnp.float32)
        row = row_ids(16)
        for step in range(DMIN):
            total = jnp.sum(spikes[step].astype(jnp.float32), axis=0, keepdims=True)
            counts = jnp.where(row == number * DMIN + step, total, counts)
        if not last:
            rest[-2][...] = counts
        else:
            total = jnp.sum(counts, axis=1, keepdims=True)
            total = jnp.where(row == lane_ids(16), total, 0.0)
            total = jnp.sum(total, axis=0, keepdims=True)
            total = jnp.broadcast_to(total, (8, BLOCK))
            for copy in range(pk_out.shape[0] // 8):
                pk_out[pl.ds(8 * copy, 8), :] = total

    return body


def rates_body(counts_ref, area_ref, v_ref, out_ref, v_out):
    v_out[...] = v_ref[...]
    counts = counts_ref[...]
    blocks = counts.shape[0]
    table = (area_ref[...] == row_ids(BLOCK, blocks)).astype(jnp.float32)
    sizes = jnp.sum(table, axis=1, keepdims=True) * float(TRIALS * BLOCK)
    table = table.astype(jnp.bfloat16)
    high = jnp.floor(counts * (1.0 / 128.0))
    low = counts - high * 128.0
    sums = [
        jnp.dot(table, part.astype(jnp.bfloat16), preferred_element_type=jnp.float32)
        for part in (high, low)
    ]
    rates = (sums[0] * 128.0 + sums[1]) / sizes
    out_ref[...] = jnp.transpose(rates)[:STEPS, :AREAS]


def exchanged(copies, groups):
    rows = copies.shape[0]
    peers = len(groups[0])
    pieces = copies.reshape(peers, 1, rows // peers * BLOCK)
    got = lax.all_to_all(
        pieces, "device", split_axis=0, concat_axis=0, axis_index_groups=groups
    )
    return got.reshape(rows, BLOCK)


def on_device(
    initial_bits, membrane, drive, leak_shift, weights, pre_block, block_mask, delay, area_of_block
):
    words = jax.ShapeDtypeStruct((HALF, BLOCK), jnp.int32)
    volts = jax.ShapeDtypeStruct((TRIALS, BLOCK), jnp.float32)
    totals = jax.ShapeDtypeStruct((16, BLOCK), jnp.float32)
    sums = jax.ShapeDtypeStruct((DMIN * TRIALS, BLOCK), jnp.float32)
    blocks = area_of_block.shape[0]
    table = pltpu.VMEM((NDELAY * TABLE + 8, BLOCK), jnp.int32)
    codes = jax.ShapeDtypeStruct((PLAN, SLOTS), jnp.int32)

    flat = weights.reshape(SLOTS * BLOCK, BLOCK)
    drive = drive.reshape(1, BLOCK)
    leak_shift = leak_shift.reshape(1, BLOCK)
    v = membrane
    counts = []
    bits = jnp.transpose(initial_bits, (0, 2, 1)).reshape(8, TRIALS)
    first_input = jnp.pad(bits, ((0, 8), (0, BLOCK - TRIALS)))
    device = lax.broadcast(lax.axis_index("device"), (1, BLOCK))
    for row, values in enumerate((pre_block, block_mask, delay, device), 8):
        first_input = jnp.where(row_ids(16) == row, values, first_input)
    copies, early_plan, late_plan = kernel_call(
        first_body,
        (words, codes, codes),
        [VMEM],
        [],
        "first",
        8,
        pl.CostEstimate(flops=10**10, bytes_accessed=1 << 18, transcendentals=0),
    )(first_input)
    own, other = [], []
    devices = range(lax.axis_size("device"))
    chips = [sorted((d for d in devices if d // CORE % 2 == c), key=chip_order) for c in range(2)]
    for number in range(STEPS // DMIN):
        mine = exchanged(copies, chips)
        theirs = lax.ppermute(mine, "device", [(d, d ^ CORE) for d in devices])
        own = [mine] + own[:2]
        n_hist = len(own)
        early = kernel_call(
            early_body(n_hist), sums, [VMEM] + [VMEM] * (2 * n_hist), [table], "early", 24
        )(early_plan, *own, *other[: n_hist - 1], flat)
        other = [theirs] + other[:2]
        last = number == STEPS // DMIN - 1
        out = jax.ShapeDtypeStruct((blocks, BLOCK), jnp.float32) if last else words
        rest = [*other[:2], flat, early, v, drive, leak_shift, *counts]
        v, copies, *counts = kernel_call(
            late_body(number, n_hist),
            (volts, out) if last else (volts, out, totals),
            [VMEM] + [VMEM] * len(rest),
            [table],
            "late",
            24,
        )(late_plan, *rest)
    everyone = exchanged(copies, [list(devices)])
    rates = jax.ShapeDtypeStruct((STEPS, AREAS), jnp.float32)
    rates, v = kernel_call(rates_body, (rates, volts), [VMEM] * 3, [], "rates", 8)(
        everyone, area_of_block.reshape(1, blocks), v
    )
    return v, rates


def solution(mesh):
    split = P("device")
    columns = P(None, "device")
    return jax.shard_map(
        on_device,
        mesh=Mesh(mesh.devices.reshape(-1), ("device",)),
        in_specs=(
            P(None, None, "device"),
            columns,
            split,
            split,
            split,
            split,
            split,
            split,
            P(),
        ),
        out_specs=(columns, P()),
        check_vma=False,
    )
```

```python
import jax
import jax.numpy as jnp
from jax import lax
from jax.experimental import pallas as pl
from jax.experimental.pallas import tpu as pltpu
from jax.sharding import Mesh
from jax.sharding import PartitionSpec as P

AREAS = 32
DMIN = 2
NDELAY = 4
STEPS = 10
BLOCK = 128
TRIALS = 48
SLOTS = 128
THRESHOLD = 200.0
EARLY, LATE = 48, 40
PLAN = 160
WORDS = 3
HALF = 128 * WORDS
TABLE = 2 * HALF
CORE = 8

VMEM = pl.BlockSpec(memory_space=pltpu.VMEM)
ANY = pl.BlockSpec(memory_space=pl.ANY)


def kernel_call(body, outs, ins, scratch, name, limit, cost=None):
    return pl.pallas_call(
        body,
        out_shape=outs,
        in_specs=ins,
        out_specs=jax.tree.map(lambda _: VMEM, outs),
        scratch_shapes=scratch,
        name=name,
        cost_estimate=cost,
        compiler_params=pltpu.CompilerParams(vmem_limit_bytes=limit << 20),
    )


def row_ids(rows, lanes=BLOCK):
    return lax.broadcasted_iota(jnp.int32, (rows, lanes), 0)


def lane_ids(rows, lanes=BLOCK):
    return lax.broadcasted_iota(jnp.int32, (rows, lanes), 1)


def words_of(spikes):
    words = []
    for j in range(WORDS):
        bits = jnp.zeros((8, BLOCK), jnp.int32)
        for step in range(DMIN):
            for part in range(2):
                shift = row_ids(8) + (8 * part + 16 * step)
                flags = spikes[step][16 * j + 8 * part : 16 * j + 8 * part + 8]
                bits = bits | jnp.where(flags, jnp.left_shift(1, shift), 0)
        words.append(jnp.sum(bits, axis=0, keepdims=True, dtype=jnp.int32))
    return words


def store_copies(out_ref, words):
    which = row_ids(24) % WORDS
    rows = jnp.where(which == 0, words[0], jnp.where(which == 1, words[1], words[2]))
    for copy in range(HALF // 24):
        out_ref[pl.ds(24 * copy, 24), :] = rows


def first_body(input_ref, out_ref):
    trial = lane_ids(8, TRIALS)
    which = row_ids(8, TRIALS)
    place = jnp.left_shift(1, trial % 16).astype(jnp.float32)
    places = jnp.where(trial // 16 == which, place, 0.0).astype(jnp.bfloat16)
    packed = jnp.zeros((8, BLOCK), jnp.int32)
    shift = row_ids(32, TRIALS)
    for step in range(DMIN):
        bits = [
            jnp.bitwise_and(jnp.right_shift(input_ref[4 * step + w : 4 * step + w + 1, :TRIALS], shift), 1)
            for w in range(BLOCK // 32)
        ]
        bits = jnp.concatenate(bits, axis=0).astype(jnp.float32).astype(jnp.bfloat16)
        half = lax.dot_general(
            places, bits, (((1,), (1,)), ((), ())), preferred_element_type=jnp.float32
        )
        packed = packed | jnp.left_shift(half.astype(jnp.int32), 16 * step)
    store_copies(out_ref, [packed[j : j + 1] for j in range(WORDS)])


def team(block):
    return (block // 64 + block // 16 + block + block // CORE) % 2


def place(block):
    z = (block + 7 + team(block)) % 8
    return (block // 16 % 4 * 8 + z) * 4 + block // 64


def slot_codes(pre, mask, delay, device):
    lag = delay - DMIN
    other = jnp.bitwise_xor(team(pre), team(device))
    base = lag * TABLE + other * HALF + place(pre) * WORDS
    late = jnp.where((other == 1) & (lag < 2), 1, 0)
    kind = jnp.where(mask == 1, late, 2)
    return kind * (1 << 20) + base * SLOTS + lane_ids(1)


def plan_body(input_ref, after_ref, *out_refs):
    slots = slot_codes(*[input_ref[8 + i : 9 + i, :] for i in range(4)])
    kind = jnp.broadcast_to(jnp.right_shift(slots, 20), (SLOTS, SLOTS))
    code = jnp.bitwise_and(slots, (1 << 20) - 1)
    sub, lane = row_ids(SLOTS), lane_ids(SLOTS)
    before = jnp.where((jnp.transpose(kind) == kind) & (sub < lane), 1, 0)
    rank = jnp.sum(before, axis=0, keepdims=True, dtype=jnp.int32)
    nothing = NDELAY * TABLE * SLOTS
    for k, out_ref in enumerate(out_refs):
        hit = (kind == k) & (rank == sub)
        codes = jnp.sum(jnp.where(hit, code - nothing, 0), axis=1, keepdims=True, dtype=jnp.int32)
        count = jnp.where(kind == k, 1, 0)
        count = jnp.sum(count, axis=1, keepdims=True, dtype=jnp.int32)
        codes = codes + nothing + jnp.where(sub == 0, jnp.left_shift(count, 20), 0)
        out_ref[pl.ds(0, SLOTS), :] = codes
        out_ref[pl.ds(SLOTS, PLAN - SLOTS), :] = jnp.full((PLAN - SLOTS, SLOTS), nothing, jnp.int32)


def shifted(older, newer):
    low = 0 if older is None else lax.shift_right_logical(older, 16)
    return low | jnp.left_shift(newer, 16)


def fill(table, lag, half, newer, older):
    at = pl.ds(lag * TABLE + half * HALF, HALF)
    if newer is None:
        table[at, :] = jnp.zeros((HALF, BLOCK), jnp.int32)
    elif lag % 2:
        table[at, :] = shifted(None if older is None else older[...], newer[...])
    else:
        table[at, :] = newer[...]


def arrivals(plan_ref, size, table, w_ref):
    table[pl.ds(NDELAY * TABLE, 8), :] = jnp.zeros((8, BLOCK), jnp.int32)
    mask = jnp.left_shift(1, row_ids(32))

    def group(i, acc):
        left, right = [], []
        for k in range(size):
            code = plan_ref[i * size + k, 0]
            base = jnp.bitwise_and(jnp.right_shift(code, 7), (1 << 13) - 1)
            slot = jnp.bitwise_and(code, SLOTS - 1)
            rows = []
            for j in range(WORDS):
                word = table[pl.ds(base + j, 1), :]
                bit = jnp.bitwise_and(word, mask)
                rows.append(bit.astype(jnp.float32).astype(jnp.bfloat16))
            left.append(jnp.concatenate(rows, axis=0))
            right.append(w_ref[pl.ds(pl.multiple_of(slot * BLOCK, BLOCK), BLOCK), :])
        left = jnp.concatenate(left, axis=1)
        right = jnp.concatenate(right, axis=0)
        return acc + jnp.dot(left, right, preferred_element_type=jnp.float32)

    zero = jnp.zeros((DMIN * TRIALS, BLOCK), jnp.float32)
    count = jnp.right_shift(plan_ref[0, 0], 20)
    groups = sum((count > i).astype(jnp.int32) for i in range(0, SLOTS, size))
    return lax.fori_loop(0, groups, group, zero)


def early_body(n_hist):
    def body(plan_ref, *refs):
        own = list(refs[:n_hist]) + [None] * (3 - n_hist)
        other = list(refs[n_hist : 2 * n_hist - 1]) + [None] * (3 - n_hist)
        w_ref, out_ref, table = refs[2 * n_hist - 1 :]
        for lag in range(NDELAY):
            a = lag // 2
            fill(table, lag, 0, own[a], own[a + 1] if a < 2 else None)
            if lag >= 2:
                fill(table, lag, 1, other[a - 1], other[a] if a < 2 else None)
        out_ref[...] = arrivals(plan_ref, EARLY, table, w_ref)

    return body


def late_body(number, n_hist):
    last = number == STEPS // DMIN - 1

    def body(plan_ref, *refs):
        newer = refs[0]
        older = refs[1] if n_hist > 1 else None
        rest = refs[min(n_hist, 2) :]
        w_ref, early_ref, v_ref, drive_ref, leak_ref = rest[:5]
        count_ref = rest[5] if number else None
        v_out, pk_out = rest[-3 - (not last) : -1 - (not last)]
        table = rest[-1]

        for lag in range(2):
            fill(table, lag, 1, newer, older)
        current = early_ref[...] + arrivals(plan_ref, LATE, table, w_ref)
        bit = row_ids(32)
        power = jnp.left_shift(1, jnp.maximum(30 - bit, 0)).astype(jnp.float32)
        scale = jnp.where(bit == 31, -(2.0**-31), power * 2.0**-30)

        v = v_ref[...]
        if number == 0:
            v = jnp.floor(v)
        drive = drive_ref[...].astype(jnp.float32)
        leak = 1.0 / jnp.left_shift(jnp.ones((1, BLOCK), jnp.int32), leak_ref[...]).astype(jnp.float32)
        spikes = []
        for step in range(DMIN):
            arrived = jnp.concatenate(
                [
                    current[32 * j + 16 * step : 32 * j + 16 * step + 16]
                    * scale[16 * step : 16 * step + 16]
                    for j in range(WORDS)
                ],
                axis=0,
            )
            v = v - jnp.floor(v * leak) + arrived + drive
            fired = v >= THRESHOLD
            v = jnp.where(fired, 0.0, jnp.maximum(v, -THRESHOLD))
            spikes.append(fired)
        v_out[...] = v
        if not last:
            store_copies(pk_out, words_of(spikes))
        counts = count_ref[...] if number else jnp.zeros((16, BLOCK), jnp.float32)
        row = row_ids(16)
        for step in range(DMIN):
            total = jnp.sum(spikes[step].astype(jnp.float32), axis=0, keepdims=True)
            counts = jnp.where(row == number * DMIN + step, total, counts)
        if not last:
            rest[-2][...] = counts
        else:
            total = jnp.sum(counts, axis=1, keepdims=True)
            total = jnp.where(row == lane_ids(16), total, 0.0)
            total = jnp.sum(total, axis=0, keepdims=True)
            total = jnp.broadcast_to(total, (8, BLOCK))
            for copy in range(pk_out.shape[0] // 8):
                pk_out[pl.ds(8 * copy, 8), :] = total

    return body


def rates_body(counts_ref, area_ref, v_ref, out_ref, v_out):
    v_out[...] = v_ref[...]
    counts = counts_ref[...]
    blocks = counts.shape[0]
    table = (area_ref[...] == row_ids(BLOCK, blocks)).astype(jnp.float32)
    sizes = jnp.sum(table, axis=1, keepdims=True) * float(TRIALS * BLOCK)
    table = table.astype(jnp.bfloat16)
    high = jnp.floor(counts * (1.0 / 128.0))
    low = counts - high * 128.0
    sums = [
        jnp.dot(table, part.astype(jnp.bfloat16), preferred_element_type=jnp.float32)
        for part in (high, low)
    ]
    rates = (sums[0] * 128.0 + sums[1]) / sizes
    out_ref[...] = jnp.transpose(rates)[:STEPS, :AREAS]


def exchanged(copies, groups):
    rows = copies.shape[0]
    peers = len(groups[0])
    pieces = copies.reshape(peers, 1, rows // peers * BLOCK)
    got = lax.all_to_all(
        pieces, "device", split_axis=0, concat_axis=0, axis_index_groups=groups
    )
    return got.reshape(rows, BLOCK)


def on_device(
    initial_bits, membrane, drive, leak_shift, weights, pre_block, block_mask, delay, area_of_block
):
    words = jax.ShapeDtypeStruct((HALF, BLOCK), jnp.int32)
    volts = jax.ShapeDtypeStruct((TRIALS, BLOCK), jnp.float32)
    totals = jax.ShapeDtypeStruct((16, BLOCK), jnp.float32)
    sums = jax.ShapeDtypeStruct((DMIN * TRIALS, BLOCK), jnp.float32)
    blocks = area_of_block.shape[0]
    table = pltpu.VMEM((NDELAY * TABLE + 8, BLOCK), jnp.int32)
    codes = jax.ShapeDtypeStruct((PLAN, SLOTS), jnp.int32)

    flat = weights.reshape(SLOTS * BLOCK, BLOCK)
    drive = drive.reshape(1, BLOCK)
    leak_shift = leak_shift.reshape(1, BLOCK)
    v = membrane
    counts = []
    bits = jnp.transpose(initial_bits, (0, 2, 1)).reshape(8, TRIALS)
    first_input = jnp.pad(bits, ((0, 8), (0, BLOCK - TRIALS)))
    device = lax.broadcast(lax.axis_index("device"), (1, BLOCK))
    for row, values in enumerate((pre_block, block_mask, delay, device), 8):
        first_input = jnp.where(row_ids(16) == row, values, first_input)
    cost = pl.CostEstimate(flops=10**10, bytes_accessed=1 << 18, transcendentals=0)
    copies = kernel_call(first_body, words, [VMEM], [], "first", 8, cost)(first_input)
    own, other = [], []
    devices = range(lax.axis_size("device"))
    teams = [sorted((d for d in devices if team(d) == t), key=place) for t in range(2)]
    for number in range(STEPS // DMIN):
        mine = exchanged(copies, teams)
        theirs = lax.ppermute(mine, "device", [(d, d ^ CORE) for d in devices])
        if number == 0:
            early_plan, late_plan = kernel_call(
                plan_body, (codes, codes), [VMEM, ANY], [], "plan", 8
            )(first_input, mine)
        own = [mine] + own[:2]
        n_hist = len(own)
        early = kernel_call(
            early_body(n_hist), sums, [VMEM] + [VMEM] * (2 * n_hist), [table], "early", 24
        )(early_plan, *own, *other[: n_hist - 1], flat)
        other = [theirs] + other[:2]
        last = number == STEPS // DMIN - 1
        out = jax.ShapeDtypeStruct((blocks, BLOCK), jnp.float32) if last else words
        rest = [*other[:2], flat, early, v, drive, leak_shift, *counts]
        v, copies, *counts = kernel_call(
            late_body(number, n_hist),
            (volts, out) if last else (volts, out, totals),
            [VMEM] + [VMEM] * len(rest),
            [table],
            "late",
            24,
        )(late_plan, *rest)
    everyone = exchanged(copies, [list(devices)])
    rates = jax.ShapeDtypeStruct((STEPS, AREAS), jnp.float32)
    rates, v = kernel_call(rates_body, (rates, volts), [VMEM] * 3, [], "rates", 8)(
        everyone, area_of_block.reshape(1, blocks), v
    )
    return v, rates


def solution(mesh):
    split = P("device")
    columns = P(None, "device")
    return jax.shard_map(
        on_device,
        mesh=Mesh(mesh.devices.reshape(-1), ("device",)),
        in_specs=(
            P(None, None, "device"),
            columns,
            split,
            split,
            split,
            split,
            split,
            split,
            P(),
        ),
        out_specs=(columns, P()),
        check_vma=False,
    )
```

```python
import jax
import jax.numpy as jnp
from jax import lax
from jax.experimental import pallas as pl
from jax.experimental.pallas import tpu as pltpu
from jax.sharding import Mesh
from jax.sharding import PartitionSpec as P

AREAS = 32
DMIN = 2
NDELAY = 4
STEPS = 10
BLOCK = 128
TRIALS = 48
SLOTS = 128
THRESHOLD = 200.0
EARLY, LATE = 48, 40
PLAN = 160
WORDS = 3
HALF = 128 * WORDS
TABLE = 2 * HALF
CORE = 8

VMEM = pl.BlockSpec(memory_space=pltpu.VMEM)
ANY = pl.BlockSpec(memory_space=pl.ANY)


def kernel_call(body, outs, ins, scratch, name, limit, cost=None):
    return pl.pallas_call(
        body,
        out_shape=outs,
        in_specs=ins,
        out_specs=jax.tree.map(lambda _: VMEM, outs),
        scratch_shapes=scratch,
        name=name,
        cost_estimate=cost,
        compiler_params=pltpu.CompilerParams(vmem_limit_bytes=limit << 20),
    )


def row_ids(rows, lanes=BLOCK):
    return lax.broadcasted_iota(jnp.int32, (rows, lanes), 0)


def lane_ids(rows, lanes=BLOCK):
    return lax.broadcasted_iota(jnp.int32, (rows, lanes), 1)


def words_of(spikes):
    words = []
    for j in range(WORDS):
        bits = jnp.zeros((8, BLOCK), jnp.int32)
        for step in range(DMIN):
            for part in range(2):
                shift = row_ids(8) + (8 * part + 16 * step)
                flags = spikes[step][16 * j + 8 * part : 16 * j + 8 * part + 8]
                bits = bits | jnp.where(flags, jnp.left_shift(1, shift), 0)
        words.append(jnp.sum(bits, axis=0, keepdims=True, dtype=jnp.int32))
    return words


def store_copies(out_ref, words):
    which = row_ids(24) % WORDS
    rows = jnp.where(which == 0, words[0], jnp.where(which == 1, words[1], words[2]))
    for copy in range(HALF // 24):
        out_ref[pl.ds(24 * copy, 24), :] = rows


def first_body(input_ref, out_ref):
    trial = lane_ids(8, TRIALS)
    which = row_ids(8, TRIALS)
    place = jnp.left_shift(1, trial % 16).astype(jnp.float32)
    places = jnp.where(trial // 16 == which, place, 0.0).astype(jnp.bfloat16)
    packed = jnp.zeros((8, BLOCK), jnp.int32)
    shift = row_ids(32, TRIALS)
    for step in range(DMIN):
        bits = [
            jnp.bitwise_and(jnp.right_shift(input_ref[4 * step + w : 4 * step + w + 1, :TRIALS], shift), 1)
            for w in range(BLOCK // 32)
        ]
        bits = jnp.concatenate(bits, axis=0).astype(jnp.float32).astype(jnp.bfloat16)
        half = lax.dot_general(
            places, bits, (((1,), (1,)), ((), ())), preferred_element_type=jnp.float32
        )
        packed = packed | jnp.left_shift(half.astype(jnp.int32), 16 * step)
    store_copies(out_ref, [packed[j : j + 1] for j in range(WORDS)])


def team(block):
    return (block // 32 + block // CORE) % 2


def place(block):
    return (block // 16 % 4 * 8 + block % 8) * 4 + block // 64


def slot_codes(pre, mask, delay, device):
    lag = delay - DMIN
    other = jnp.bitwise_xor(team(pre), team(device))
    base = lag * TABLE + other * HALF + place(pre) * WORDS
    late = jnp.where((other == 1) & (lag < 2), 1, 0)
    kind = jnp.where(mask == 1, late, 2)
    return kind * (1 << 20) + base * SLOTS + lane_ids(1)


def plan_body(input_ref, after_ref, *out_refs):
    slots = slot_codes(*[input_ref[8 + i : 9 + i, :] for i in range(4)])
    kind = jnp.broadcast_to(jnp.right_shift(slots, 20), (SLOTS, SLOTS))
    code = jnp.bitwise_and(slots, (1 << 20) - 1)
    sub, lane = row_ids(SLOTS), lane_ids(SLOTS)
    before = jnp.where((jnp.transpose(kind) == kind) & (sub < lane), 1, 0)
    rank = jnp.sum(before, axis=0, keepdims=True, dtype=jnp.int32)
    nothing = NDELAY * TABLE * SLOTS
    for k, out_ref in enumerate(out_refs):
        hit = (kind == k) & (rank == sub)
        codes = jnp.sum(jnp.where(hit, code - nothing, 0), axis=1, keepdims=True, dtype=jnp.int32)
        count = jnp.where(kind == k, 1, 0)
        count = jnp.sum(count, axis=1, keepdims=True, dtype=jnp.int32)
        codes = codes + nothing + jnp.where(sub == 0, jnp.left_shift(count, 20), 0)
        out_ref[pl.ds(0, SLOTS), :] = codes
        out_ref[pl.ds(SLOTS, PLAN - SLOTS), :] = jnp.full((PLAN - SLOTS, SLOTS), nothing, jnp.int32)


def shifted(older, newer):
    low = 0 if older is None else lax.shift_right_logical(older, 16)
    return low | jnp.left_shift(newer, 16)


def fill(table, lag, half, newer, older):
    at = pl.ds(lag * TABLE + half * HALF, HALF)
    if newer is None:
        table[at, :] = jnp.zeros((HALF, BLOCK), jnp.int32)
    elif lag % 2:
        table[at, :] = shifted(None if older is None else older[...], newer[...])
    else:
        table[at, :] = newer[...]


def arrivals(plan_ref, size, table, w_ref):
    table[pl.ds(NDELAY * TABLE, 8), :] = jnp.zeros((8, BLOCK), jnp.int32)
    mask = jnp.left_shift(1, row_ids(32))

    def group(i, acc):
        left, right = [], []
        for k in range(size):
            code = plan_ref[i * size + k, 0]
            base = jnp.bitwise_and(jnp.right_shift(code, 7), (1 << 13) - 1)
            slot = jnp.bitwise_and(code, SLOTS - 1)
            rows = []
            for j in range(WORDS):
                word = table[pl.ds(base + j, 1), :]
                bit = jnp.bitwise_and(word, mask)
                rows.append(bit.astype(jnp.float32).astype(jnp.bfloat16))
            left.append(jnp.concatenate(rows, axis=0))
            right.append(w_ref[pl.ds(pl.multiple_of(slot * BLOCK, BLOCK), BLOCK), :])
        left = jnp.concatenate(left, axis=1)
        right = jnp.concatenate(right, axis=0)
        return acc + jnp.dot(left, right, preferred_element_type=jnp.float32)

    zero = jnp.zeros((DMIN * TRIALS, BLOCK), jnp.float32)
    count = jnp.right_shift(plan_ref[0, 0], 20)
    groups = sum((count > i).astype(jnp.int32) for i in range(0, SLOTS, size))
    return lax.fori_loop(0, groups, group, zero)


def early_body(n_hist):
    def body(plan_ref, *refs):
        own = list(refs[:n_hist]) + [None] * (3 - n_hist)
        other = list(refs[n_hist : 2 * n_hist - 1]) + [None] * (3 - n_hist)
        w_ref, out_ref, table = refs[2 * n_hist - 1 :]
        for lag in range(NDELAY):
            a = lag // 2
            fill(table, lag, 0, own[a], own[a + 1] if a < 2 else None)
            if lag >= 2:
                fill(table, lag, 1, other[a - 1], other[a] if a < 2 else None)
        out_ref[...] = arrivals(plan_ref, EARLY, table, w_ref)

    return body


def late_body(number, n_hist):
    last = number == STEPS // DMIN - 1

    def body(plan_ref, *refs):
        newer = refs[0]
        older = refs[1] if n_hist > 1 else None
        rest = refs[min(n_hist, 2) :]
        w_ref, early_ref, v_ref, drive_ref, leak_ref = rest[:5]
        count_ref = rest[5] if number else None
        v_out, pk_out = rest[-3 - (not last) : -1 - (not last)]
        table = rest[-1]

        for lag in range(2):
            fill(table, lag, 1, newer, older)
        current = early_ref[...] + arrivals(plan_ref, LATE, table, w_ref)
        bit = row_ids(32)
        power = jnp.left_shift(1, jnp.maximum(30 - bit, 0)).astype(jnp.float32)
        scale = jnp.where(bit == 31, -(2.0**-31), power * 2.0**-30)

        v = v_ref[...]
        if number == 0:
            v = jnp.floor(v)
        drive = drive_ref[...].astype(jnp.float32)
        leak = 1.0 / jnp.left_shift(jnp.ones((1, BLOCK), jnp.int32), leak_ref[...]).astype(jnp.float32)
        spikes = []
        for step in range(DMIN):
            arrived = jnp.concatenate(
                [
                    current[32 * j + 16 * step : 32 * j + 16 * step + 16]
                    * scale[16 * step : 16 * step + 16]
                    for j in range(WORDS)
                ],
                axis=0,
            )
            v = v - jnp.floor(v * leak) + arrived + drive
            fired = v >= THRESHOLD
            v = jnp.where(fired, 0.0, jnp.maximum(v, -THRESHOLD))
            spikes.append(fired)
        v_out[...] = v
        if not last:
            store_copies(pk_out, words_of(spikes))
        counts = count_ref[...] if number else jnp.zeros((16, BLOCK), jnp.float32)
        row = row_ids(16)
        for step in range(DMIN):
            total = jnp.sum(spikes[step].astype(jnp.float32), axis=0, keepdims=True)
            counts = jnp.where(row == number * DMIN + step, total, counts)
        if not last:
            rest[-2][...] = counts
        else:
            total = jnp.sum(counts, axis=1, keepdims=True)
            total = jnp.where(row == lane_ids(16), total, 0.0)
            total = jnp.sum(total, axis=0, keepdims=True)
            total = jnp.broadcast_to(total, (8, BLOCK))
            for copy in range(pk_out.shape[0] // 8):
                pk_out[pl.ds(8 * copy, 8), :] = total

    return body


def rates_body(counts_ref, area_ref, v_ref, out_ref, v_out):
    v_out[...] = v_ref[...]
    counts = counts_ref[...]
    blocks = counts.shape[0]
    table = (area_ref[...] == row_ids(BLOCK, blocks)).astype(jnp.float32)
    sizes = jnp.sum(table, axis=1, keepdims=True) * float(TRIALS * BLOCK)
    table = table.astype(jnp.bfloat16)
    high = jnp.floor(counts * (1.0 / 128.0))
    low = counts - high * 128.0
    sums = [
        jnp.dot(table, part.astype(jnp.bfloat16), preferred_element_type=jnp.float32)
        for part in (high, low)
    ]
    rates = (sums[0] * 128.0 + sums[1]) / sizes
    out_ref[...] = jnp.transpose(rates)[:STEPS, :AREAS]


def exchanged(copies, groups):
    rows = copies.shape[0]
    peers = len(groups[0])
    pieces = copies.reshape(peers, 1, rows // peers * BLOCK)
    got = lax.all_to_all(
        pieces, "device", split_axis=0, concat_axis=0, axis_index_groups=groups
    )
    return got.reshape(rows, BLOCK)


def on_device(
    initial_bits, membrane, drive, leak_shift, weights, pre_block, block_mask, delay, area_of_block
):
    words = jax.ShapeDtypeStruct((HALF, BLOCK), jnp.int32)
    volts = jax.ShapeDtypeStruct((TRIALS, BLOCK), jnp.float32)
    totals = jax.ShapeDtypeStruct((16, BLOCK), jnp.float32)
    sums = jax.ShapeDtypeStruct((DMIN * TRIALS, BLOCK), jnp.float32)
    blocks = area_of_block.shape[0]
    table = pltpu.VMEM((NDELAY * TABLE + 8, BLOCK), jnp.int32)
    codes = jax.ShapeDtypeStruct((PLAN, SLOTS), jnp.int32)

    flat = weights.reshape(SLOTS * BLOCK, BLOCK)
    drive = drive.reshape(1, BLOCK)
    leak_shift = leak_shift.reshape(1, BLOCK)
    v = membrane
    counts = []
    bits = jnp.transpose(initial_bits, (0, 2, 1)).reshape(8, TRIALS)
    first_input = jnp.pad(bits, ((0, 8), (0, BLOCK - TRIALS)))
    device = lax.broadcast(lax.axis_index("device"), (1, BLOCK))
    for row, values in enumerate((pre_block, block_mask, delay, device), 8):
        first_input = jnp.where(row_ids(16) == row, values, first_input)
    cost = pl.CostEstimate(flops=10**10, bytes_accessed=1 << 18, transcendentals=0)
    copies = kernel_call(first_body, words, [VMEM], [], "first", 8, cost)(first_input)
    own, other = [], []
    devices = range(lax.axis_size("device"))
    teams = [sorted((d for d in devices if team(d) == t), key=place) for t in range(2)]
    for number in range(STEPS // DMIN):
        mine = exchanged(copies, teams)
        theirs = lax.ppermute(mine, "device", [(d, d ^ CORE) for d in devices])
        if number == 0:
            early_plan, late_plan = kernel_call(
                plan_body, (codes, codes), [VMEM, ANY], [], "plan", 8
            )(first_input, mine)
        own = [mine] + own[:2]
        n_hist = len(own)
        early = kernel_call(
            early_body(n_hist), sums, [VMEM] + [VMEM] * (2 * n_hist), [table], "early", 24
        )(early_plan, *own, *other[: n_hist - 1], flat)
        other = [theirs] + other[:2]
        last = number == STEPS // DMIN - 1
        out = jax.ShapeDtypeStruct((blocks, BLOCK), jnp.float32) if last else words
        rest = [*other[:2], flat, early, v, drive, leak_shift, *counts]
        v, copies, *counts = kernel_call(
            late_body(number, n_hist),
            (volts, out) if last else (volts, out, totals),
            [VMEM] + [VMEM] * len(rest),
            [table],
            "late",
            24,
        )(late_plan, *rest)
    everyone = exchanged(copies, [list(devices)])
    rates = jax.ShapeDtypeStruct((STEPS, AREAS), jnp.float32)
    rates, v = kernel_call(rates_body, (rates, volts), [VMEM] * 3, [], "rates", 8)(
        everyone, area_of_block.reshape(1, blocks), v
    )
    return v, rates


def solution(mesh):
    split = P("device")
    columns = P(None, "device")
    return jax.shard_map(
        on_device,
        mesh=Mesh(mesh.devices.reshape(-1), ("device",)),
        in_specs=(
            P(None, None, "device"),
            columns,
            split,
            split,
            split,
            split,
            split,
            split,
            P(),
        ),
        out_specs=(columns, P()),
        check_vma=False,
    )
```

```python
import jax
import jax.numpy as jnp
from jax import lax
from jax.experimental import pallas as pl
from jax.experimental.pallas import tpu as pltpu
from jax.sharding import Mesh
from jax.sharding import PartitionSpec as P

AREAS = 32
DMIN = 2
NDELAY = 4
STEPS = 10
BLOCK = 128
TRIALS = 48
SLOTS = 128
THRESHOLD = 200.0
EARLY, LATE = 48, 40
PLAN = 160
WORDS = 3
HALF = 128 * WORDS
TABLE = 2 * HALF
CORE = 8

VMEM = pl.BlockSpec(memory_space=pltpu.VMEM)
ANY = pl.BlockSpec(memory_space=pl.ANY)


def kernel_call(body, outs, ins, scratch, name, limit, cost=None):
    return pl.pallas_call(
        body,
        out_shape=outs,
        in_specs=ins,
        out_specs=jax.tree.map(lambda _: VMEM, outs),
        scratch_shapes=scratch,
        name=name,
        cost_estimate=cost,
        compiler_params=pltpu.CompilerParams(vmem_limit_bytes=limit << 20),
    )


def row_ids(rows, lanes=BLOCK):
    return lax.broadcasted_iota(jnp.int32, (rows, lanes), 0)


def lane_ids(rows, lanes=BLOCK):
    return lax.broadcasted_iota(jnp.int32, (rows, lanes), 1)


def words_of(spikes):
    words = []
    for j in range(WORDS):
        bits = jnp.zeros((8, BLOCK), jnp.int32)
        for step in range(DMIN):
            for part in range(2):
                shift = row_ids(8) + (8 * part + 16 * step)
                flags = spikes[step][16 * j + 8 * part : 16 * j + 8 * part + 8]
                bits = bits | jnp.where(flags, jnp.left_shift(1, shift), 0)
        words.append(jnp.sum(bits, axis=0, keepdims=True, dtype=jnp.int32))
    return words


def store_copies(out_ref, words):
    which = row_ids(24) % WORDS
    rows = jnp.where(which == 0, words[0], jnp.where(which == 1, words[1], words[2]))
    for copy in range(HALF // 24):
        out_ref[pl.ds(24 * copy, 24), :] = rows


def first_body(input_ref, out_ref):
    trial = lane_ids(8, TRIALS)
    which = row_ids(8, TRIALS)
    place = jnp.left_shift(1, trial % 16).astype(jnp.float32)
    places = jnp.where(trial // 16 == which, place, 0.0).astype(jnp.bfloat16)
    packed = jnp.zeros((8, BLOCK), jnp.int32)
    shift = row_ids(32, TRIALS)
    for step in range(DMIN):
        bits = [
            jnp.bitwise_and(jnp.right_shift(input_ref[4 * step + w : 4 * step + w + 1, :TRIALS], shift), 1)
            for w in range(BLOCK // 32)
        ]
        bits = jnp.concatenate(bits, axis=0).astype(jnp.float32).astype(jnp.bfloat16)
        half = lax.dot_general(
            places, bits, (((1,), (1,)), ((), ())), preferred_element_type=jnp.float32
        )
        packed = packed | jnp.left_shift(half.astype(jnp.int32), 16 * step)
    store_copies(out_ref, [packed[j : j + 1] for j in range(WORDS)])


def team(block):
    return block // CORE % 2


def chip_key(block):
    y, x, z = block // 64, block // 16 % 4, block % 8
    hops = y - 2 * (y // 3) + x - 2 * (x // 3) + z - z // 4 * (2 * z - 8)
    return (9 - hops) % 9 * 128 + (y * 8 + z) * 4 + x


def place(block):
    chip = row_ids(128)
    keys = chip_key(chip // 8 * 16 + chip % 8)
    return jnp.sum((keys < chip_key(block)).astype(jnp.int32), axis=0, keepdims=True, dtype=jnp.int32)


def slot_codes(pre, mask, delay, device):
    lag = delay - DMIN
    other = jnp.bitwise_xor(team(pre), team(device))
    base = lag * TABLE + other * HALF + place(pre) * WORDS
    late = jnp.where((other == 1) & (lag < 2), 1, 0)
    kind = jnp.where(mask == 1, late, 2)
    return kind * (1 << 20) + base * SLOTS + lane_ids(1)


def plan_body(input_ref, after_ref, *out_refs):
    slots = slot_codes(*[input_ref[8 + i : 9 + i, :] for i in range(4)])
    kind = jnp.broadcast_to(jnp.right_shift(slots, 20), (SLOTS, SLOTS))
    code = jnp.bitwise_and(slots, (1 << 20) - 1)
    sub, lane = row_ids(SLOTS), lane_ids(SLOTS)
    before = jnp.where((jnp.transpose(kind) == kind) & (sub < lane), 1, 0)
    rank = jnp.sum(before, axis=0, keepdims=True, dtype=jnp.int32)
    nothing = NDELAY * TABLE * SLOTS
    for k, out_ref in enumerate(out_refs):
        hit = (kind == k) & (rank == sub)
        codes = jnp.sum(jnp.where(hit, code - nothing, 0), axis=1, keepdims=True, dtype=jnp.int32)
        count = jnp.where(kind == k, 1, 0)
        count = jnp.sum(count, axis=1, keepdims=True, dtype=jnp.int32)
        codes = codes + nothing + jnp.where(sub == 0, jnp.left_shift(count, 20), 0)
        out_ref[pl.ds(0, SLOTS), :] = codes
        out_ref[pl.ds(SLOTS, PLAN - SLOTS), :] = jnp.full((PLAN - SLOTS, SLOTS), nothing, jnp.int32)


def shifted(older, newer):
    low = 0 if older is None else lax.shift_right_logical(older, 16)
    return low | jnp.left_shift(newer, 16)


def fill(table, lag, half, newer, older):
    at = pl.ds(lag * TABLE + half * HALF, HALF)
    if newer is None:
        table[at, :] = jnp.zeros((HALF, BLOCK), jnp.int32)
    elif lag % 2:
        table[at, :] = shifted(None if older is None else older[...], newer[...])
    else:
        table[at, :] = newer[...]


def arrivals(plan_ref, size, table, w_ref):
    table[pl.ds(NDELAY * TABLE, 8), :] = jnp.zeros((8, BLOCK), jnp.int32)
    mask = jnp.left_shift(1, row_ids(32))

    def group(i, acc):
        left, right = [], []
        for k in range(size):
            code = plan_ref[i * size + k, 0]
            base = jnp.bitwise_and(jnp.right_shift(code, 7), (1 << 13) - 1)
            slot = jnp.bitwise_and(code, SLOTS - 1)
            rows = []
            for j in range(WORDS):
                word = table[pl.ds(base + j, 1), :]
                bit = jnp.bitwise_and(word, mask)
                rows.append(bit.astype(jnp.float32).astype(jnp.bfloat16))
            left.append(jnp.concatenate(rows, axis=0))
            right.append(w_ref[pl.ds(pl.multiple_of(slot * BLOCK, BLOCK), BLOCK), :])
        left = jnp.concatenate(left, axis=1)
        right = jnp.concatenate(right, axis=0)
        return acc + jnp.dot(left, right, preferred_element_type=jnp.float32)

    zero = jnp.zeros((DMIN * TRIALS, BLOCK), jnp.float32)
    count = jnp.right_shift(plan_ref[0, 0], 20)
    groups = sum((count > i).astype(jnp.int32) for i in range(0, SLOTS, size))
    return lax.fori_loop(0, groups, group, zero)


def early_body(n_hist):
    def body(plan_ref, *refs):
        own = list(refs[:n_hist]) + [None] * (3 - n_hist)
        other = list(refs[n_hist : 2 * n_hist - 1]) + [None] * (3 - n_hist)
        w_ref, out_ref, table = refs[2 * n_hist - 1 :]
        for lag in range(NDELAY):
            a = lag // 2
            fill(table, lag, 0, own[a], own[a + 1] if a < 2 else None)
            if lag >= 2:
                fill(table, lag, 1, other[a - 1], other[a] if a < 2 else None)
        out_ref[...] = arrivals(plan_ref, EARLY, table, w_ref)

    return body


def late_body(number, n_hist):
    last = number == STEPS // DMIN - 1

    def body(plan_ref, *refs):
        newer = refs[0]
        older = refs[1] if n_hist > 1 else None
        rest = refs[min(n_hist, 2) :]
        w_ref, early_ref, v_ref, drive_ref, leak_ref = rest[:5]
        count_ref = rest[5] if number else None
        v_out, pk_out = rest[-3 - (not last) : -1 - (not last)]
        table = rest[-1]

        for lag in range(2):
            fill(table, lag, 1, newer, older)
        current = early_ref[...] + arrivals(plan_ref, LATE, table, w_ref)
        bit = row_ids(32)
        power = jnp.left_shift(1, jnp.maximum(30 - bit, 0)).astype(jnp.float32)
        scale = jnp.where(bit == 31, -(2.0**-31), power * 2.0**-30)

        v = v_ref[...]
        if number == 0:
            v = jnp.floor(v)
        drive = drive_ref[...].astype(jnp.float32)
        leak = 1.0 / jnp.left_shift(jnp.ones((1, BLOCK), jnp.int32), leak_ref[...]).astype(jnp.float32)
        spikes = []
        for step in range(DMIN):
            arrived = jnp.concatenate(
                [
                    current[32 * j + 16 * step : 32 * j + 16 * step + 16]
                    * scale[16 * step : 16 * step + 16]
                    for j in range(WORDS)
                ],
                axis=0,
            )
            v = v - jnp.floor(v * leak) + arrived + drive
            fired = v >= THRESHOLD
            v = jnp.where(fired, 0.0, jnp.maximum(v, -THRESHOLD))
            spikes.append(fired)
        v_out[...] = v
        if not last:
            store_copies(pk_out, words_of(spikes))
        counts = count_ref[...] if number else jnp.zeros((16, BLOCK), jnp.float32)
        row = row_ids(16)
        for step in range(DMIN):
            total = jnp.sum(spikes[step].astype(jnp.float32), axis=0, keepdims=True)
            counts = jnp.where(row == number * DMIN + step, total, counts)
        if not last:
            rest[-2][...] = counts
        else:
            total = jnp.sum(counts, axis=1, keepdims=True)
            total = jnp.where(row == lane_ids(16), total, 0.0)
            total = jnp.sum(total, axis=0, keepdims=True)
            total = jnp.broadcast_to(total, (8, BLOCK))
            for copy in range(pk_out.shape[0] // 8):
                pk_out[pl.ds(8 * copy, 8), :] = total

    return body


def rates_body(counts_ref, area_ref, v_ref, out_ref, v_out):
    v_out[...] = v_ref[...]
    counts = counts_ref[...]
    blocks = counts.shape[0]
    table = (area_ref[...] == row_ids(BLOCK, blocks)).astype(jnp.float32)
    sizes = jnp.sum(table, axis=1, keepdims=True) * float(TRIALS * BLOCK)
    table = table.astype(jnp.bfloat16)
    high = jnp.floor(counts * (1.0 / 128.0))
    low = counts - high * 128.0
    sums = [
        jnp.dot(table, part.astype(jnp.bfloat16), preferred_element_type=jnp.float32)
        for part in (high, low)
    ]
    rates = (sums[0] * 128.0 + sums[1]) / sizes
    out_ref[...] = jnp.transpose(rates)[:STEPS, :AREAS]


def exchanged(copies, groups):
    rows = copies.shape[0]
    peers = len(groups[0])
    pieces = copies.reshape(peers, 1, rows // peers * BLOCK)
    got = lax.all_to_all(
        pieces, "device", split_axis=0, concat_axis=0, axis_index_groups=groups
    )
    return got.reshape(rows, BLOCK)


def on_device(
    initial_bits, membrane, drive, leak_shift, weights, pre_block, block_mask, delay, area_of_block
):
    words = jax.ShapeDtypeStruct((HALF, BLOCK), jnp.int32)
    volts = jax.ShapeDtypeStruct((TRIALS, BLOCK), jnp.float32)
    totals = jax.ShapeDtypeStruct((16, BLOCK), jnp.float32)
    sums = jax.ShapeDtypeStruct((DMIN * TRIALS, BLOCK), jnp.float32)
    blocks = area_of_block.shape[0]
    table = pltpu.VMEM((NDELAY * TABLE + 8, BLOCK), jnp.int32)
    codes = jax.ShapeDtypeStruct((PLAN, SLOTS), jnp.int32)

    flat = weights.reshape(SLOTS * BLOCK, BLOCK)
    drive = drive.reshape(1, BLOCK)
    leak_shift = leak_shift.reshape(1, BLOCK)
    v = membrane
    counts = []
    bits = jnp.transpose(initial_bits, (0, 2, 1)).reshape(8, TRIALS)
    first_input = jnp.pad(bits, ((0, 8), (0, BLOCK - TRIALS)))
    device = lax.broadcast(lax.axis_index("device"), (1, BLOCK))
    for row, values in enumerate((pre_block, block_mask, delay, device), 8):
        first_input = jnp.where(row_ids(16) == row, values, first_input)
    cost = pl.CostEstimate(flops=10**10, bytes_accessed=1 << 18, transcendentals=0)
    copies = kernel_call(first_body, words, [VMEM], [], "first", 8, cost)(first_input)
    own, other = [], []
    devices = range(lax.axis_size("device"))
    teams = [sorted((d for d in devices if team(d) == t), key=chip_key) for t in range(2)]
    for number in range(STEPS // DMIN):
        mine = exchanged(copies, teams)
        theirs = lax.ppermute(mine, "device", [(d, d ^ CORE) for d in devices])
        if number == 0:
            early_plan, late_plan = kernel_call(
                plan_body, (codes, codes), [VMEM, ANY], [], "plan", 8
            )(first_input, mine)
        own = [mine] + own[:2]
        n_hist = len(own)
        early = kernel_call(
            early_body(n_hist), sums, [VMEM] + [VMEM] * (2 * n_hist), [table], "early", 24
        )(early_plan, *own, *other[: n_hist - 1], flat)
        other = [theirs] + other[:2]
        last = number == STEPS // DMIN - 1
        out = jax.ShapeDtypeStruct((blocks, BLOCK), jnp.float32) if last else words
        rest = [*other[:2], flat, early, v, drive, leak_shift, *counts]
        v, copies, *counts = kernel_call(
            late_body(number, n_hist),
            (volts, out) if last else (volts, out, totals),
            [VMEM] + [VMEM] * len(rest),
            [table],
            "late",
            24,
        )(late_plan, *rest)
    everyone = exchanged(copies, [list(devices)])
    rates = jax.ShapeDtypeStruct((STEPS, AREAS), jnp.float32)
    rates, v = kernel_call(rates_body, (rates, volts), [VMEM] * 3, [], "rates", 8)(
        everyone, area_of_block.reshape(1, blocks), v
    )
    return v, rates


def solution(mesh):
    split = P("device")
    columns = P(None, "device")
    return jax.shard_map(
        on_device,
        mesh=Mesh(mesh.devices.reshape(-1), ("device",)),
        in_specs=(
            P(None, None, "device"),
            columns,
            split,
            split,
            split,
            split,
            split,
            split,
            P(),
        ),
        out_specs=(columns, P()),
        check_vma=False,
    )
```

```python
import jax
import jax.numpy as jnp
from jax import lax
from jax.experimental import pallas as pl
from jax.experimental.pallas import tpu as pltpu
from jax.sharding import Mesh
from jax.sharding import PartitionSpec as P

AREAS = 32
DMIN = 2
NDELAY = 4
STEPS = 10
BLOCK = 128
TRIALS = 48
SLOTS = 128
THRESHOLD = 200.0
EARLY, LATE = 48, 40
PLAN = 160
WORDS = 3
HALF = 128 * WORDS
TABLE = 2 * HALF
CORE = 8

VMEM = pl.BlockSpec(memory_space=pltpu.VMEM)
ANY = pl.BlockSpec(memory_space=pl.ANY)


def kernel_call(body, outs, ins, scratch, name, limit, cost=None):
    return pl.pallas_call(
        body,
        out_shape=outs,
        in_specs=ins,
        out_specs=jax.tree.map(lambda _: VMEM, outs),
        scratch_shapes=scratch,
        name=name,
        cost_estimate=cost,
        compiler_params=pltpu.CompilerParams(vmem_limit_bytes=limit << 20),
    )


def row_ids(rows, lanes=BLOCK):
    return lax.broadcasted_iota(jnp.int32, (rows, lanes), 0)


def lane_ids(rows, lanes=BLOCK):
    return lax.broadcasted_iota(jnp.int32, (rows, lanes), 1)


def words_of(spikes):
    words = []
    for j in range(WORDS):
        bits = jnp.zeros((8, BLOCK), jnp.int32)
        for step in range(DMIN):
            for part in range(2):
                shift = row_ids(8) + (8 * part + 16 * step)
                flags = spikes[step][16 * j + 8 * part : 16 * j + 8 * part + 8]
                bits = bits | jnp.where(flags, jnp.left_shift(1, shift), 0)
        words.append(jnp.sum(bits, axis=0, keepdims=True, dtype=jnp.int32))
    return words


def store_copies(out_ref, words):
    which = row_ids(24) % WORDS
    rows = jnp.where(which == 0, words[0], jnp.where(which == 1, words[1], words[2]))
    for copy in range(HALF // 24):
        out_ref[pl.ds(24 * copy, 24), :] = rows


def first_body(input_ref, out_ref):
    trial = lane_ids(8, TRIALS)
    which = row_ids(8, TRIALS)
    place = jnp.left_shift(1, trial % 16).astype(jnp.float32)
    places = jnp.where(trial // 16 == which, place, 0.0).astype(jnp.bfloat16)
    packed = jnp.zeros((8, BLOCK), jnp.int32)
    shift = row_ids(32, TRIALS)
    for step in range(DMIN):
        bits = [
            jnp.bitwise_and(jnp.right_shift(input_ref[4 * step + w : 4 * step + w + 1, :TRIALS], shift), 1)
            for w in range(BLOCK // 32)
        ]
        bits = jnp.concatenate(bits, axis=0).astype(jnp.float32).astype(jnp.bfloat16)
        half = lax.dot_general(
            places, bits, (((1,), (1,)), ((), ())), preferred_element_type=jnp.float32
        )
        packed = packed | jnp.left_shift(half.astype(jnp.int32), 16 * step)
    store_copies(out_ref, [packed[j : j + 1] for j in range(WORDS)])


def team(block):
    return block // CORE % 2


def chip_key(block):
    y, x, z = block // 64, block // 16 % 4, block % 8
    hops = y - 2 * (y // 3) + x - 2 * (x // 3) + z - z // 4 * (2 * z - 8)
    return (9 - hops) % 9 * 128 + (y * 8 + z) * 4 + x


def column(row):
    return jnp.transpose(jnp.broadcast_to(row, (BLOCK, BLOCK)))


def place(block):
    chip = lane_ids(1)
    keys = column(chip_key(chip // 8 * 16 + chip % 8))
    return jnp.sum((keys < chip_key(block)).astype(jnp.int32), axis=0, keepdims=True, dtype=jnp.int32)


def slot_codes(pre, mask, delay, device):
    lag = delay - DMIN
    other = jnp.bitwise_xor(team(pre), team(device))
    base = lag * TABLE + other * HALF + place(pre) * WORDS
    late = jnp.where((other == 1) & (lag < 2), 1, 0)
    kind = jnp.where(mask == 1, late, 2)
    return kind * (1 << 20) + base * SLOTS + lane_ids(1)


def plan_body(input_ref, after_ref, *out_refs):
    slots = slot_codes(*[input_ref[8 + i : 9 + i, :] for i in range(4)])
    kind = jnp.broadcast_to(jnp.right_shift(slots, 20), (SLOTS, SLOTS))
    code = jnp.bitwise_and(slots, (1 << 20) - 1)
    sub, lane = row_ids(SLOTS), lane_ids(SLOTS)
    before = jnp.where((column(kind[:1]) == kind) & (sub < lane), 1, 0)
    rank = jnp.sum(before, axis=0, keepdims=True, dtype=jnp.int32)
    nothing = NDELAY * TABLE * SLOTS
    for k, out_ref in enumerate(out_refs):
        hit = (kind == k) & (rank == sub)
        codes = jnp.sum(jnp.where(hit, code - nothing, 0), axis=1, keepdims=True, dtype=jnp.int32)
        count = jnp.where(kind == k, 1, 0)
        count = jnp.sum(count, axis=1, keepdims=True, dtype=jnp.int32)
        codes = codes + nothing + jnp.where(sub == 0, jnp.left_shift(count, 20), 0)
        out_ref[pl.ds(0, SLOTS), :] = codes
        out_ref[pl.ds(SLOTS, PLAN - SLOTS), :] = jnp.full((PLAN - SLOTS, SLOTS), nothing, jnp.int32)


def shifted(older, newer):
    low = 0 if older is None else lax.shift_right_logical(older, 16)
    return low | jnp.left_shift(newer, 16)


def fill(table, lag, half, newer, older):
    at = pl.ds(lag * TABLE + half * HALF, HALF)
    if newer is None:
        table[at, :] = jnp.zeros((HALF, BLOCK), jnp.int32)
    elif lag % 2:
        table[at, :] = shifted(None if older is None else older[...], newer[...])
    else:
        table[at, :] = newer[...]


def arrivals(plan_ref, size, table, w_ref):
    table[pl.ds(NDELAY * TABLE, 8), :] = jnp.zeros((8, BLOCK), jnp.int32)
    mask = jnp.left_shift(1, row_ids(32))

    def group(i, acc):
        left, right = [], []
        for k in range(size):
            code = plan_ref[i * size + k, 0]
            base = jnp.bitwise_and(jnp.right_shift(code, 7), (1 << 13) - 1)
            slot = jnp.bitwise_and(code, SLOTS - 1)
            rows = []
            for j in range(WORDS):
                word = table[pl.ds(base + j, 1), :]
                bit = jnp.bitwise_and(word, mask)
                rows.append(bit.astype(jnp.float32).astype(jnp.bfloat16))
            left.append(jnp.concatenate(rows, axis=0))
            right.append(w_ref[pl.ds(pl.multiple_of(slot * BLOCK, BLOCK), BLOCK), :])
        left = jnp.concatenate(left, axis=1)
        right = jnp.concatenate(right, axis=0)
        return acc + jnp.dot(left, right, preferred_element_type=jnp.float32)

    zero = jnp.zeros((DMIN * TRIALS, BLOCK), jnp.float32)
    count = jnp.right_shift(plan_ref[0, 0], 20)
    groups = sum((count > i).astype(jnp.int32) for i in range(0, SLOTS, size))
    return lax.fori_loop(0, groups, group, zero)


def early_body(n_hist):
    def body(plan_ref, *refs):
        own = list(refs[:n_hist]) + [None] * (3 - n_hist)
        other = list(refs[n_hist : 2 * n_hist - 1]) + [None] * (3 - n_hist)
        w_ref, out_ref, table = refs[2 * n_hist - 1 :]
        for lag in range(NDELAY):
            a = lag // 2
            fill(table, lag, 0, own[a], own[a + 1] if a < 2 else None)
            if lag >= 2:
                fill(table, lag, 1, other[a - 1], other[a] if a < 2 else None)
        out_ref[...] = arrivals(plan_ref, EARLY, table, w_ref)

    return body


def late_body(number, n_hist):
    last = number == STEPS // DMIN - 1

    def body(plan_ref, *refs):
        newer = refs[0]
        older = refs[1] if n_hist > 1 else None
        rest = refs[min(n_hist, 2) :]
        w_ref, early_ref, v_ref, drive_ref, leak_ref = rest[:5]
        count_ref = rest[5] if number else None
        v_out, pk_out = rest[-3 - (not last) : -1 - (not last)]
        table = rest[-1]

        for lag in range(2):
            fill(table, lag, 1, newer, older)
        current = early_ref[...] + arrivals(plan_ref, LATE, table, w_ref)
        bit = row_ids(32)
        power = jnp.left_shift(1, jnp.maximum(30 - bit, 0)).astype(jnp.float32)
        scale = jnp.where(bit == 31, -(2.0**-31), power * 2.0**-30)

        v = v_ref[...]
        if number == 0:
            v = jnp.floor(v)
        drive = drive_ref[...].astype(jnp.float32)
        leak = 1.0 / jnp.left_shift(jnp.ones((1, BLOCK), jnp.int32), leak_ref[...]).astype(jnp.float32)
        spikes = []
        for step in range(DMIN):
            arrived = jnp.concatenate(
                [
                    current[32 * j + 16 * step : 32 * j + 16 * step + 16]
                    * scale[16 * step : 16 * step + 16]
                    for j in range(WORDS)
                ],
                axis=0,
            )
            v = v - jnp.floor(v * leak) + arrived + drive
            fired = v >= THRESHOLD
            v = jnp.where(fired, 0.0, jnp.maximum(v, -THRESHOLD))
            spikes.append(fired)
        v_out[...] = v
        if not last:
            store_copies(pk_out, words_of(spikes))
        counts = count_ref[...] if number else jnp.zeros((16, BLOCK), jnp.float32)
        row = row_ids(16)
        for step in range(DMIN):
            total = jnp.sum(spikes[step].astype(jnp.float32), axis=0, keepdims=True)
            counts = jnp.where(row == number * DMIN + step, total, counts)
        if not last:
            rest[-2][...] = counts
        else:
            total = jnp.sum(counts, axis=1, keepdims=True)
            total = jnp.where(row == lane_ids(16), total, 0.0)
            total = jnp.sum(total, axis=0, keepdims=True)
            total = jnp.broadcast_to(total, (8, BLOCK))
            for copy in range(pk_out.shape[0] // 8):
                pk_out[pl.ds(8 * copy, 8), :] = total

    return body


def rates_body(counts_ref, area_ref, v_ref, out_ref, v_out):
    v_out[...] = v_ref[...]
    counts = counts_ref[...]
    blocks = counts.shape[0]
    table = (area_ref[...] == row_ids(BLOCK, blocks)).astype(jnp.float32)
    sizes = jnp.sum(table, axis=1, keepdims=True) * float(TRIALS * BLOCK)
    table = table.astype(jnp.bfloat16)
    high = jnp.floor(counts * (1.0 / 128.0))
    low = counts - high * 128.0
    sums = [
        jnp.dot(table, part.astype(jnp.bfloat16), preferred_element_type=jnp.float32)
        for part in (high, low)
    ]
    rates = (sums[0] * 128.0 + sums[1]) / sizes
    out_ref[...] = jnp.transpose(rates)[:STEPS, :AREAS]


def exchanged(copies, groups):
    rows = copies.shape[0]
    peers = len(groups[0])
    pieces = copies.reshape(peers, 1, rows // peers * BLOCK)
    got = lax.all_to_all(
        pieces, "device", split_axis=0, concat_axis=0, axis_index_groups=groups
    )
    return got.reshape(rows, BLOCK)


def on_device(
    initial_bits, membrane, drive, leak_shift, weights, pre_block, block_mask, delay, area_of_block
):
    words = jax.ShapeDtypeStruct((HALF, BLOCK), jnp.int32)
    volts = jax.ShapeDtypeStruct((TRIALS, BLOCK), jnp.float32)
    totals = jax.ShapeDtypeStruct((16, BLOCK), jnp.float32)
    sums = jax.ShapeDtypeStruct((DMIN * TRIALS, BLOCK), jnp.float32)
    blocks = area_of_block.shape[0]
    table = pltpu.VMEM((NDELAY * TABLE + 8, BLOCK), jnp.int32)
    codes = jax.ShapeDtypeStruct((PLAN, SLOTS), jnp.int32)

    flat = weights.reshape(SLOTS * BLOCK, BLOCK)
    drive = drive.reshape(1, BLOCK)
    leak_shift = leak_shift.reshape(1, BLOCK)
    v = membrane
    counts = []
    bits = jnp.transpose(initial_bits, (0, 2, 1)).reshape(8, TRIALS)
    first_input = jnp.pad(bits, ((0, 8), (0, BLOCK - TRIALS)))
    device = lax.broadcast(lax.axis_index("device"), (1, BLOCK))
    for row, values in enumerate((pre_block, block_mask, delay, device), 8):
        first_input = jnp.where(row_ids(16) == row, values, first_input)
    cost = pl.CostEstimate(flops=10**10, bytes_accessed=1 << 18, transcendentals=0)
    copies = kernel_call(first_body, words, [VMEM], [], "first", 8, cost)(first_input)
    own, other = [], []
    devices = range(lax.axis_size("device"))
    teams = [sorted((d for d in devices if team(d) == t), key=chip_key) for t in range(2)]
    for number in range(STEPS // DMIN):
        mine = exchanged(copies, teams)
        theirs = lax.ppermute(mine, "device", [(d, d ^ CORE) for d in devices])
        if number == 0:
            early_plan, late_plan = kernel_call(
                plan_body, (codes, codes), [VMEM, ANY], [], "plan", 8
            )(first_input, mine)
        own = [mine] + own[:2]
        n_hist = len(own)
        early = kernel_call(
            early_body(n_hist), sums, [VMEM] + [VMEM] * (2 * n_hist), [table], "early", 24
        )(early_plan, *own, *other[: n_hist - 1], flat)
        other = [theirs] + other[:2]
        last = number == STEPS // DMIN - 1
        out = jax.ShapeDtypeStruct((blocks, BLOCK), jnp.float32) if last else words
        rest = [*other[:2], flat, early, v, drive, leak_shift, *counts]
        v, copies, *counts = kernel_call(
            late_body(number, n_hist),
            (volts, out) if last else (volts, out, totals),
            [VMEM] + [VMEM] * len(rest),
            [table],
            "late",
            24,
        )(late_plan, *rest)
    everyone = exchanged(copies, [list(devices)])
    rates = jax.ShapeDtypeStruct((STEPS, AREAS), jnp.float32)
    rates, v = kernel_call(rates_body, (rates, volts), [VMEM] * 3, [], "rates", 8)(
        everyone, area_of_block.reshape(1, blocks), v
    )
    return v, rates


def solution(mesh):
    split = P("device")
    columns = P(None, "device")
    return jax.shard_map(
        on_device,
        mesh=Mesh(mesh.devices.reshape(-1), ("device",)),
        in_specs=(
            P(None, None, "device"),
            columns,
            split,
            split,
            split,
            split,
            split,
            split,
            P(),
        ),
        out_specs=(columns, P()),
        check_vma=False,
    )
```
